32 devices in a mesh: batch: 4 (over z), tensor: 8 (over y, x, core).
Axes of the slice: x: 2, y: 2, z: 4, core: 2. Of those that a mesh axis runs over, the one named last changes fastest.
Arguments:
- attn_values: bfloat16 [1024, 8192], P('batch', 'tensor'), may hold values from -6 to 6
- out_weight: bfloat16 [8192, 8192], P('tensor'), may hold values from -0.09375 to 0.09375
- residual_t: bfloat16 [8192, 1024], P('tensor', 'batch'), may hold values from -6 to 6
- projector: bfloat16 [8192, 4096], P('tensor'), may hold values from -0.0625 to 0.0625
- student_input: bfloat16 [1024, 4096], P('batch', 'tensor'), may hold values from -6 to 6
- norm_gain: float32 [4096], replicated, may hold values from 0.1 to 1.9
- w_gate: bfloat16 [4096, 8192], P('batch', 'tensor'), may hold values from -0.09375 to 0.09375
- w_up: bfloat16 [4096, 8192], P('batch', 'tensor'), may hold values from -0.09375 to 0.09375
- w_down: bfloat16 [4096, 8192], P('batch', 'tensor'), may hold values from -0.0625 to 0.0625
- route_index: int32 [4, 64], P('batch'), may hold values from -1 to 255, as said below
Outputs:
- teacher_hidden: bfloat16 [8192, 1024], P('tensor', 'batch')
- grad_gate: float32 [4096, 8192], P('batch', 'tensor')
- grad_up: float32 [4096, 8192], P('batch', 'tensor')
- grad_down: float32 [4096, 8192], P('batch', 'tensor')
The draws below stay inside these ranges and needn't reach their ends.
Inputs may be any that keep to these rules, and one draw needn't show every extreme that they name: `route_index`: in each batch group the live slots come first, hold distinct positions in increasing order, and the empty slots after them hold -1. The batch groups hold 128 live slots together, and some batch group has all 64 slots live.
All inputs are finite; a program needn't handle non-finite values.
Results may differ from the reference program's by a relative error of at most 0.025.
Values may be sent and summed in bfloat16 or wider, within the bound.
A program may use at most 128 MiB of HBM per device.

```python
import math
import jax
import jax.numpy as jnp
from jax import lax

DT = 8192
D = 4096
FF = 8192
TOK = 256
CAP = 32
CAPMAX = 64
ROUTED = 128
TOKENS = 1024
N_BATCH = 4
N_TENSOR = 8


def draw_route_index(key, part):
    key_perm, key_spread, key_pos = jax.random.split(jax.random.fold_in(key, 71), 3)
    half_groups = N_BATCH // 2
    spread = jax.random.randint(key_spread, (half_groups,), 0, CAP + 1)
    spread = spread.at[0].set(CAP)
    counts = jnp.concatenate([CAP + spread, CAP - spread])
    order_groups = jax.random.permutation(key_perm, N_BATCH)
    counts = counts[order_groups]
    group_keys = jax.random.split(key_pos, N_BATCH)

    def one_group(group_key, live_count):
        shuffled = jax.random.permutation(group_key, TOK)[:CAPMAX]
        slot_ids = jnp.arange(CAPMAX, dtype=jnp.int32)
        chosen = jnp.where(slot_ids < live_count, shuffled, TOK)
        chosen = jnp.sort(chosen)
        return jnp.where(slot_ids < live_count, chosen, -1)
    return jax.vmap(one_group)(group_keys, counts).astype(jnp.int32)


def raised(array, stream_key, source, target, blocks, factor):
    owner, partner = [(jnp.arange(array.shape[dim]) // (array.shape[dim] // blocks)).reshape([-1 if axis == dim else 1 for axis in range(array.ndim)]) for dim in (source, target)]
    chosen = jax.random.permutation(stream_key, blocks)[partner]
    strong = (owner == chosen) | (owner == (partner + blocks // 2) % blocks)
    return jnp.where(strong, factor * array, array)


def steps_of(key, shape, shards, least, high):
    loudness, own = 1.0, jax.random.fold_in(key, 6)
    for position, shards_of in shards:
        heights = jnp.exp(jax.random.uniform(jax.random.fold_in(own, position), (shards_of,), jnp.float32, least / len(shards), high / len(shards)))
        loudness = loudness * jnp.repeat(heights, shape[position] // shards_of).reshape([-1 if axis == position else 1 for axis in range(len(shape))])
    return loudness


def bell_draw(own_key, shape, deviation, reach, cuts=(), kind=jnp.bfloat16):
    level = steps_of(own_key, shape, cuts, -0.22, 0.18) if cuts else 1.0
    values = jax.random.normal(own_key, shape, jnp.float32) * deviation * level
    return jnp.minimum(jnp.maximum(values, -reach), reach).astype(kind)


def gaussian_with(own_key, extent, scale, limit, shards, heavy, kind=jnp.bfloat16):
    drawn = scale * jax.random.normal(own_key, extent, jnp.float32)
    if shards:
        drawn = drawn * steps_of(own_key, extent, shards, -0.22, 0.18)
    return jnp.clip(raised(drawn, jax.random.fold_in(own_key, 3), *heavy), -limit, limit).astype(kind)


def setup_inputs(seed: int = 0) -> dict:
    arg_keys = jax.random.split(jax.random.key(seed), 11)
    attn_values = bell_draw(arg_keys[0], (TOKENS, DT), 1.0, 6.0, ((0, 4), (1, 8)))
    out_weight = gaussian_with(arg_keys[1], (DT, DT), DT ** -0.5, 0.09375, ((0, 8),), (0, 1, 8, 2.0))
    residual_t = bell_draw(arg_keys[2], (DT, TOKENS), 1.0, 6.0, ((0, 8), (1, 4)))
    projector = bell_draw(arg_keys[3], (DT, D), DT ** -0.5, 0.0625, ((0, 8),))
    student_input = bell_draw(arg_keys[4], (TOKENS, D), 1.0, 6.0, ((0, 4), (1, 8)))
    norm_gain = jnp.clip(1.0 + 0.18 * jax.random.normal(arg_keys[5], (D,), jnp.float32), 0.1, 1.9)
    w_gate = bell_draw(arg_keys[6], (D, FF), D ** -0.5, 0.09375, ((0, 4), (1, 8)))
    w_up = bell_draw(arg_keys[7], (D, FF), D ** -0.5, 0.09375, ((0, 4), (1, 8)))
    w_down = bell_draw(arg_keys[8], (D, FF), FF ** -0.5, 0.0625, ((0, 4), (1, 8)))
    route_index = draw_route_index(jax.random.fold_in(arg_keys[10], 71), 0)
    return {"attn_values": attn_values, "out_weight": out_weight, "residual_t": residual_t, "projector": projector, "student_input": student_input, "norm_gain": norm_gain, "w_gate": w_gate, "w_up": w_up, "w_down": w_down, "route_index": route_index}


epsilon = 1e-05

def reference(attn_values, out_weight, residual_t, projector, student_input, norm_gain, w_gate, w_up, w_down, route_index):
    shard_width = DT // N_TENSOR

    def teacher_step(running, shard_no):
        offset = (shard_no * shard_width).astype(jnp.int32)
        columns = lax.dynamic_slice_in_dim(attn_values, offset, shard_width, 1)
        rows_block = lax.dynamic_slice_in_dim(out_weight, offset, shard_width, 0)
        partial_sum = lax.dot_general(rows_block, columns, (((0,), (1,)), ((), ())), preferred_element_type=jnp.float32)
        rounded = lax.optimization_barrier(partial_sum.astype(jnp.bfloat16))
        return (running + rounded.astype(jnp.float32), None)
    summed, _ = lax.scan(teacher_step, jnp.zeros((DT, TOKENS), jnp.float32), jnp.arange(N_TENSOR, dtype=jnp.int32))
    teacher_hidden = (residual_t.astype(jnp.float32) + summed).astype(jnp.bfloat16)
    loss_scale = 1.0 / math.sqrt(ROUTED)

    def group_step(running, group_no):
        slot_pos = lax.dynamic_index_in_dim(route_index, group_no, 0, keepdims=False)
        present = slot_pos >= 0
        safe_slot = (jnp.maximum(slot_pos, 0) + group_no * TOK).astype(jnp.int32)
        routed_teacher = jnp.where(present[None, :], jnp.take(teacher_hidden, safe_slot, axis=1), 0).astype(jnp.bfloat16)
        target = lax.dot_general(routed_teacher, projector, (((0,), (0,)), ((), ())), preferred_element_type=jnp.float32)
        routed_input = jnp.where(present[:, None], jnp.take(student_input, safe_slot, axis=0), 0).astype(jnp.float32)
        mean_square = lax.optimization_barrier(jnp.mean(routed_input * routed_input, axis=1, keepdims=True))
        normed = (routed_input * lax.rsqrt(mean_square + epsilon) * norm_gain[None, :]).astype(jnp.bfloat16)
        gate_act = jnp.dot(normed, w_gate, preferred_element_type=jnp.float32)
        up_act = jnp.dot(normed, w_up, preferred_element_type=jnp.float32)
        sigma_gate = jax.nn.sigmoid(gate_act)
        hidden = (gate_act * sigma_gate * up_act).astype(jnp.bfloat16)
        student_out = lax.dot_general(hidden, w_down, (((1,), (1,)), ((), ())), preferred_element_type=jnp.float32)
        misfit = jnp.where(present[:, None], student_out - target, 0.0)
        grad_out = (misfit * loss_scale).astype(jnp.bfloat16)
        grad_hidden = jnp.dot(grad_out, w_down, preferred_element_type=jnp.float32)
        grad_gate_act = (grad_hidden * up_act * sigma_gate * (1.0 + gate_act * (1.0 - sigma_gate))).astype(jnp.bfloat16)
        grad_up_act = (grad_hidden * gate_act * sigma_gate).astype(jnp.bfloat16)
        dims = (((0,), (0,)), ((), ()))
        gate_part = lax.dot_general(normed, grad_gate_act, dims, preferred_element_type=jnp.float32)
        up_part = lax.dot_general(normed, grad_up_act, dims, preferred_element_type=jnp.float32)
        down_part = lax.dot_general(grad_out, hidden, dims, preferred_element_type=jnp.float32)
        parts = (gate_part, up_part, down_part)
        updated = tuple((acc + lax.optimization_barrier(part.astype(jnp.bfloat16)).astype(jnp.float32) for acc, part in zip(running, parts)))
        return (updated, None)
    zero_grad = jnp.zeros((D, FF), jnp.float32)
    grads, _ = lax.scan(group_step, (zero_grad, zero_grad, zero_grad), jnp.arange(N_BATCH, dtype=jnp.int32))
    return (teacher_hidden, grads[0], grads[1], grads[2])
```

```python
import functools
import math
import types

import jax
import jax.numpy as jnp
from jax import lax
from jax.experimental import pallas as pl
from jax.experimental.pallas import tpu as pltpu
from jax.sharding import PartitionSpec as P

epsilon = 1e-05
f32 = jnp.float32
bf16 = jnp.bfloat16
VMEM = pl.BlockSpec(memory_space=pltpu.VMEM)
ANY = pl.BlockSpec(memory_space=pl.ANY)
VMEM_BYTES = 66_000_000

NAMES = (
    "attn", "out_weight", "residual", "projector", "student", "gain", "w_gate", "w_up",
    "w_down", "route", "o_rows", "o_gate", "o_up", "o_grad", "o_hidden", "o_teacher",
    "attn_v", "weight_v", "resid_v", "proj_v", "stud_v", "wg", "wu", "wd", "load_sem",
    "q_send", "q_land", "q_sem", "t_send", "t_land", "r_acc", "r_land", "f_acc", "f_land", "t_sem", "r_sem", "f_sem",
    "c_send", "c_land", "p_acc", "p_land", "p_keep", "p_send", "p_zland", "c_sem", "p_sem", "z2_sem",
    "x_land", "sq_send", "sq_land", "count_land", "x_sem", "sq_sem", "count_sem", "z_send",
    "z_land", "z_sem", "select", "rows_v", "row_sem", "gu", "gu_land", "gu_share", "gu_sem", "gh",
    "gh_land", "gh_share", "gh_sem", "part", "m_send", "m_land", "v_share", "v_land", "m_sem",
    "v_sem", "grad_v", "g_sem",
)
PROFILE = False
open_scope = []


def mark(name):
    if not PROFILE:
        return
    while open_scope:
        open_scope.pop().__exit__(None, None, None)
    if name:
        scope = jax.named_scope(name)
        scope.__enter__()
        open_scope.append(scope)


def contract(left, right, left_dim, right_dim):
    return lax.dot_general(
        left, right, (((left_dim,), (right_dim,)), ((), ())), preferred_element_type=f32
    )


def remote(src, dst, send_sem, recv_sem, **where):
    return pltpu.make_async_remote_copy(
        src_ref=src,
        dst_ref=dst,
        send_sem=send_sem,
        recv_sem=recv_sem,
        device_id=where,
        device_id_type=pl.DeviceIdType.MESH,
    )


def start_if(cond, copy):
    @pl.when(cond)
    def _():
        copy.start()


def wait_send_if(cond, copy):
    @pl.when(cond)
    def _():
        copy.wait_send()


def wait_recv_if(cond, copy):
    @pl.when(cond)
    def _():
        copy.wait_recv()


def xor(left, right, bits):
    total = 0
    for bit in range(bits):
        step = 1 << bit
        total = total + step * lax.rem(left // step + right // step, 2)
    return total


class Chain:
    def __init__(self, own, land, share, send_sem, recv_sem, me, size):
        self.own, self.land, self.share = own, land, share
        self.send_sem, self.recv_sem = send_sem, recv_sem
        self.me, self.size, self.chunks = me, size, own.shape[0]
        self.early = jnp.where(2 * me < size, 0, 1)

    def flow(self, late):
        way = 1 - self.early if late else self.early
        before = jnp.where(way == 0, self.me, self.size - 1 - self.me) > 0
        after = jnp.where(way == 0, self.size - 1 - self.me, self.me) > 0
        peer = jnp.where(way == 0, self.me + 1, self.me - 1)
        return way, before, after, peer

    def copy(self, way, chunk, peer):
        return remote(
            self.share.at[way, chunk],
            self.land.at[way, chunk],
            self.send_sem.at[way, chunk],
            self.recv_sem.at[way, chunk],
            batch=peer,
        )

    def origin(self, first, last):
        way, before, after, peer = self.flow(False)

        @pl.when(jnp.logical_not(before))
        def _():
            for chunk in range(first, last):
                self.share[way, chunk] = self.own[chunk].astype(bf16)
                self.copy(way, chunk, peer).start()

    def step(self, chunk, late):
        way, before, after, peer = self.flow(late)
        copy = self.copy(way, chunk, peer)
        wait_recv_if(before, copy)

        @pl.when(jnp.logical_and(after, before))
        def _():
            self.share[way, chunk] = (
                self.own[chunk] + self.land[way, chunk].astype(f32)
            ).astype(bf16)
            copy.start()

    def total(self, chunk):
        @pl.when(self.me > 0)
        def _():
            self.own[chunk] = self.own[chunk] + self.land[0, chunk].astype(f32)

        @pl.when(self.me < self.size - 1)
        def _():
            self.own[chunk] = self.own[chunk] + self.land[1, chunk].astype(f32)

    def drain(self):
        for late in (False, True):
            way, _, after, peer = self.flow(late)
            for chunk in range(self.chunks):
                wait_send_if(after, self.copy(way, chunk, peer))


class PlaneScatter:
    def __init__(self, acc, land, send_sem, recv_sem, chip, core, bits):
        self.acc, self.land = acc, land
        self.send_sem, self.recv_sem = send_sem, recv_sem
        self.chip, self.core, self.bits = chip, core, bits
        self.slots, self.stages = [], []
        for half in range(2):
            order = [1 << bit for bit in range(bits)]
            order = order if half == 0 else order[::-1]
            used, slots, stages = 0, {}, []
            done = 0
            for stage, flip in enumerate(order):
                moved = [
                    block
                    for block in range((1 << bits) - 1, -1, -1)
                    if block & flip and not block & done
                ]
                for block in moved:
                    slots[(stage, block ^ flip)] = used
                    used += 1
                stages.append((flip, moved))
                done |= flip
            self.slots.append(slots)
            self.stages.append(stages)

    def copy(self, half, stage, block):
        flip, _ = self.stages[half][stage]
        slot = self.slots[half][(stage, block ^ flip)]
        return remote(
            self.acc.at[block, half],
            self.land.at[slot, half],
            self.send_sem.at[slot, half],
            self.recv_sem.at[slot, half],
            tensor=2 * xor(self.chip, flip, self.bits) + self.core,
        )

    def arrived(self, half, stages, block):
        return [
            self.land[self.slots[half][(stage, block)], half].astype(f32)
            for stage in range(stages)
        ]

    def send(self, stage):
        for half in range(2):
            for block in self.stages[half][stage][1]:
                if stage:
                    value = self.acc[block, half].astype(f32)
                    for term in self.arrived(half, stage, block):
                        value = value + term
                    self.acc[block, half] = value.astype(bf16)
                self.copy(half, stage, block).start()

    def receive(self, stage):
        for half in range(2):
            for block in self.stages[half][stage][1]:
                self.copy(half, stage, block).wait_recv()

    def final(self, half):
        value = self.acc[0, half].astype(f32)
        for term in self.arrived(half, self.bits, 0):
            value = value + term
        return value

    def drain(self):
        for half in range(2):
            for stage in range(self.bits):
                for block in self.stages[half][stage][1]:
                    self.copy(half, stage, block).wait_send()


def exchange_kernel(dims, *refs):
    (groups, tensors, mean_routed) = dims
    r = types.SimpleNamespace(**dict(zip(NAMES, refs, strict=True)))

    b, t = lax.axis_index("batch"), lax.axis_index("tensor")
    chips = tensors // 2
    bits = chips.bit_length() - 1
    chip, core = t // 2, lax.rem(t, 2)
    partner = t + 1 - 2 * core
    slots = r.route.shape[1]
    tokens, heads = r.attn.shape
    feats = r.out_weight.shape[1] // tensors
    width = r.student.shape[1]
    block = r.w_gate.shape[0]
    hidden_units = r.w_gate.shape[1]
    routed = mean_routed * groups
    tall = routed // 2
    short = routed // 4
    chunks = r.gu.shape[0] // 2
    cols = hidden_units // chunks
    others = range(1, chips)

    mark("a_loads")
    loads = {}

    def load(name, src, dst):
        copy = pltpu.make_async_copy(src, dst, r.load_sem.at[len(loads)])
        copy.start()
        loads[name] = copy

    def weight_block(index):
        place = pl.multiple_of(index * feats, feats)
        return r.out_weight.at[:, pl.ds(place, feats)]

    def owner(relative, side):
        return 2 * xor(chip, relative, bits) + (core if side else 1 - core)

    load("student", r.student, r.stud_v)
    load("attn", r.attn, r.attn_v.at[pl.ds(slots, tokens)])
    for side in range(2):
        for step in range(chips):
            place = side * chips + step
            index = owner(chips - 1 - step, side)
            load(("w", place), weight_block(index), r.weight_v.at[place])
    load("w_gate", r.w_gate, r.wg)
    load("w_up", r.w_up, r.wu)
    load("residual", r.residual, r.resid_v)
    for side in range(2):
        for step in range(chips):
            place = pl.multiple_of(owner(chips - 1 - step, side) * width, width)
            load(
                ("p", side * chips + step),
                r.projector.at[:, pl.ds(place, width)],
                r.proj_v.at[side * chips + step],
            )
    load("w_down", r.w_down, r.wd)

    barrier = pltpu.get_barrier_semaphore()
    for step in others:
        pl.semaphore_signal(
            barrier,
            inc=1,
            device_id={"tensor": 2 * xor(chip, step, bits) + core},
            device_id_type=pl.DeviceIdType.MESH,
        )
    pl.semaphore_signal(
        barrier, inc=1, device_id={"tensor": partner}, device_id_type=pl.DeviceIdType.MESH
    )
    for step in range(1, groups):
        pl.semaphore_signal(
            barrier,
            inc=1,
            device_id={"batch": lax.rem(b + step, groups)},
            device_id_type=pl.DeviceIdType.MESH,
        )

    mark("b_route")
    route = r.route[...]
    row_id = lax.broadcasted_iota(jnp.int32, (slots, slots), 0)
    col_id = lax.broadcasted_iota(jnp.int32, (slots, slots), 1)
    route_col = jnp.sum(jnp.where(row_id == col_id, route, 0), axis=1, keepdims=True)
    token_id = lax.broadcasted_iota(jnp.int32, (slots, tokens), 1)
    pick = jnp.where(token_id == route_col, 1.0, 0.0).astype(bf16)
    count = jnp.sum(jnp.where(route >= 0, 1.0, 0.0), axis=1, keepdims=True)
    r.count_land[b] = jnp.broadcast_to(count, r.count_land.shape[1:])

    loads["student"].wait()
    r.x_land[0] = contract(pick, r.stud_v[...], 1, 0).astype(bf16)

    mark("c_barrier")
    pl.semaphore_wait(barrier, chips - 1 + 1 + groups - 1)

    mark("d_tprep")
    x_copies = [
        remote(
            r.x_land.at[0],
            r.x_land.at[step],
            r.x_sem.at[0, step],
            r.x_sem.at[1, step],
            tensor=2 * xor(chip, step, bits) + core,
        )
        for step in others
    ]
    for copy in x_copies[::-1]:
        copy.start()

    def count_copy(step):
        return remote(
            r.count_land.at[b],
            r.count_land.at[b],
            r.count_sem.at[0, step],
            r.count_sem.at[1, b],
            batch=lax.rem(b + step, groups),
        )

    for step in range(1, groups):
        count_copy(step).start()

    loads["attn"].wait()
    all_rows = slice(slots, slots + tokens)
    r.attn_v[0:slots] = contract(pick, r.attn_v[all_rows], 1, 0).astype(bf16)

    def pair_copy(send, land, sem, relative):
        return remote(
            send.at[relative],
            land.at[relative],
            sem.at[0, relative],
            sem.at[1, relative],
            tensor=partner,
        )

    piece = min(256, feats)

    def away(rows, send, land, sem, step):
        for place in range(0, feats, piece):
            span = slice(place, place + piece)
            value = jnp.dot(
                r.attn_v[rows], r.weight_v[step, :, span], preferred_element_type=f32
            )
            send[chips - 1 - step, :, span] = value.astype(bf16)
        pair_copy(send, land, sem, chips - 1 - step).start()

    def home(rows, send, land, sem, acc, step):
        relative = chips - 1 - step
        count = acc.shape[2]
        pair_copy(send, land, sem, relative).wait_recv()
        for place in range(0, feats, piece):
            span = slice(place, place + piece)
            value = jnp.dot(
                r.attn_v[rows], r.weight_v[chips + step, :, span], preferred_element_type=f32
            )
            value = (value + land[relative, :, span].astype(f32)).astype(bf16)
            for half in range(2):
                acc[relative, half, :, span] = value[half * count : (half + 1) * count]

    few = (slice(0, slots), r.q_send, r.q_land, r.q_sem)
    many = (all_rows, r.t_send, r.t_land, r.t_sem)
    routed_sum = PlaneScatter(
        r.r_acc, r.r_land, r.r_sem.at[0], r.r_sem.at[1], chip, core, bits
    )
    full_sum = PlaneScatter(
        r.f_acc, r.f_land, r.f_sem.at[0], r.f_sem.at[1], chip, core, bits
    )
    mark("e_away")
    for step in range(chips):
        loads[("w", step)].wait()
        away(*few, step)
    for step in range(chips):
        loads[("w", chips + step)].wait()
        home(*few, r.r_acc, step)
    routed_sum.send(0)

    mark("f_waitx")
    for copy in x_copies:
        copy.wait_recv()
    square = jnp.zeros((slots, 1), f32)
    for step in range(chips):
        value = r.x_land[step].astype(f32)
        square = square + jnp.sum(value * value, axis=1, keepdims=True)
    r.sq_send[...] = jnp.broadcast_to(square, r.sq_send.shape)
    sq_copy = remote(
        r.sq_send, r.sq_land, r.sq_sem.at[0], r.sq_sem.at[1], tensor=partner
    )
    sq_copy.start()
    away(*many, 0)
    away(*many, 1)
    mark("h_norm")
    sq_copy.wait_recv()
    square = r.sq_send[:, 0:1] + r.sq_land[:, 0:1]
    scale = lax.rsqrt(square / (width * tensors) + epsilon)

    def z_copy(relative, peer):
        return remote(
            r.z_send.at[relative],
            r.z_land.at[b],
            r.z_sem.at[0, relative],
            r.z_sem.at[1, b],
            batch=peer,
        )

    for relative in range(chips):
        peer = xor(chip, relative, bits)
        place = pl.multiple_of(peer * block + core * width, width)
        value = r.x_land[relative].astype(f32) * scale * r.gain[:, pl.ds(place, width)]
        value = value.astype(bf16)

        @pl.when(peer == b)
        def _():
            r.z_land[b] = value

        @pl.when(peer != b)
        def _():
            r.z_send[relative] = value
            z_copy(relative, peer).start()

    mark("i_home")
    for step in range(2, chips):
        away(*many, step)
    home(*many, r.f_acc, 0)
    mark("j_rrecv")
    routed_sum.receive(0)
    routed_sum.send(1)
    for stage in range(2, bits):
        routed_sum.receive(stage - 1)
        routed_sum.send(stage)
    mark("j2_home")
    for step in range(1, chips):
        home(*many, r.f_acc, step)

    mark("k_waitz")
    for group in range(groups):
        for land, sem in ((r.count_land, r.count_sem), (r.z_land, r.z_sem)):
            wait_recv_if(
                group != b,
                remote(
                    land.at[group], land.at[group], sem.at[0, 0], sem.at[1, group], batch=b
                ),
            )
    mark("l_pack")
    pack_row = lax.broadcasted_iota(jnp.int32, (routed, slots), 0).astype(f32)
    pack_col = lax.broadcasted_iota(jnp.int32, (routed, slots), 1).astype(f32)
    offset = jnp.zeros((1, 1), f32)
    packed = jnp.zeros((routed, width), f32)
    for group in range(groups):
        amount = r.count_land[group][0:1, 0:1]
        hit = jnp.logical_and(pack_col + offset == pack_row, pack_col < amount)
        r.select[group] = jnp.where(hit, 1.0, 0.0).astype(bf16)
        packed = packed + contract(r.select[group], r.z_land[group], 1, 0)
        offset = offset + amount
    r.rows_v[core] = packed.astype(bf16)
    row_copy = remote(
        r.rows_v.at[core], r.rows_v.at[core], r.row_sem.at[0], r.row_sem.at[1], tensor=partner
    )
    row_copy.start()

    mark("m_proj1")
    loads["w_gate"].wait()
    loads["w_up"].wait()

    def project(side, first):
        start = pl.multiple_of(side * width, width)
        rows = r.rows_v[side]
        for chunk in range(chunks):
            span = slice(chunk * cols, (chunk + 1) * cols)
            for which, weight in enumerate((r.wg, r.wu)):
                value = jnp.dot(
                    rows, weight[pl.ds(start, width), span], preferred_element_type=f32
                )
                for turn in range(2):
                    item = turn * chunks + chunk
                    piece = value[turn * tall : (turn + 1) * tall]
                    r.gu[item, which] = piece if first else r.gu[item, which] + piece

    project(core, True)
    mark("o_rowwait")
    remote(
        r.rows_v.at[1 - core],
        r.rows_v.at[1 - core],
        r.row_sem.at[0],
        r.row_sem.at[1],
        tensor=partner,
    ).wait_recv()
    mark("p_proj2")
    project(1 - core, False)
    gate_up = Chain(r.gu, r.gu_land, r.gu_share, r.gu_sem.at[0], r.gu_sem.at[1], b, groups)
    gate_up.origin(0, 2 * chunks)
    for side in range(2):
        r.o_rows[:, side * width : (side + 1) * width] = r.rows_v[side]

    mark("r_rrecv1")
    routed_sum.receive(bits - 1)
    loads["residual"].wait()
    routed_resid = contract(pick, r.resid_v[...], 1, 1)
    for half in range(2):
        first = half * (slots // 2)
        value = routed_sum.final(half) + routed_resid[first : first + slots // 2]
        r.p_keep[first : first + slots // 2] = value.astype(bf16)

    def target_copy(relative):
        return pair_copy(r.c_send, r.c_land, r.c_sem, relative)

    mark("s_target")
    for step in range(chips):
        relative = chips - 1 - step
        loads[("p", step)].wait()
        value = jnp.dot(r.p_keep[...], r.proj_v[step], preferred_element_type=f32)
        r.c_send[relative] = value.astype(bf16)
        target_copy(relative).start()
    target_sum = PlaneScatter(
        r.p_acc, r.p_land, r.p_sem.at[0], r.p_sem.at[1], chip, core, bits
    )

    def target_home():
        mark("u_target2")
        for step in range(chips):
            relative = chips - 1 - step
            loads[("p", chips + step)].wait()
            value = jnp.dot(r.p_keep[...], r.proj_v[chips + step], preferred_element_type=f32)
            target_copy(relative).wait_recv()
            value = (value + r.c_land[relative].astype(f32)).astype(bf16)
            for half in range(2):
                first = half * (slots // 2)
                r.p_acc[relative, half] = value[first : first + slots // 2]
        target_sum.send(0)

    def target_relay():
        mark("v_trelay")
        for stage in range(1, bits):
            target_sum.receive(stage - 1)
            target_sum.send(stage)
        full_sum.send(0)

    home_plane = chip == b

    def target_z(peer):
        return remote(
            r.p_send, r.p_zland.at[b], r.z2_sem.at[0], r.z2_sem.at[1 + b], batch=peer
        )

    def target_end():
        mark("x_tz")
        target_sum.receive(bits - 1)
        for half in range(2):
            first = half * (slots // 2)
            value = target_sum.final(half).astype(bf16)

            @pl.when(home_plane)
            def _():
                r.p_zland[b, first : first + slots // 2] = value

            @pl.when(jnp.logical_not(home_plane))
            def _():
                r.p_send[first : first + slots // 2] = value

        start_if(jnp.logical_not(home_plane), target_z(chip))

    def down(turn):
        mark(f"y_down{turn}")
        rows = slice(turn * tall, (turn + 1) * tall)
        if turn == 0:
            loads["w_down"].wait()
        for chunk in range(chunks):
            item = turn * chunks + chunk
            gate_up.total(item)
            gate, up = r.gu[item, 0], r.gu[item, 1]
            value = (gate * jax.nn.sigmoid(gate) * up).astype(bf16)
            r.o_hidden[rows, chunk * cols : (chunk + 1) * cols] = value
        r.part[turn] = contract(r.o_hidden[rows], r.wd[...], 1, 1)

        mark(f"z_tarrive{turn}")

        @pl.when(home_plane)
        def _():
            value = jnp.zeros((tall, width), f32)
            for group in range(groups):
                if turn == 0:
                    wait_recv_if(
                        group != b,
                        remote(
                            r.p_zland.at[group],
                            r.p_zland.at[group],
                            r.z2_sem.at[0],
                            r.z2_sem.at[1 + group],
                            batch=b,
                        ),
                    )
                value = value + contract(r.select[group, rows], r.p_zland[group], 1, 0)
            span = pl.ds(pl.multiple_of(core * width, width), width)
            r.part[turn, :, span] = r.part[turn, :, span] - value

    kept = pl.ds(pl.multiple_of(core * short, short), short)
    given = pl.ds(pl.multiple_of((1 - core) * short, short), short)
    half_cols = block // 2
    loss_scale = 1.0 / math.sqrt(routed)

    def misfit_copy(turn):
        return remote(
            r.m_send.at[turn],
            r.m_land.at[turn],
            r.m_sem.at[0, turn],
            r.m_sem.at[1, turn],
            tensor=partner,
        )

    def double_copy(turn, stage, half):
        bit = stage if half == 0 else bits - 1 - stage
        return remote(
            r.v_share.at[turn, stage, half],
            r.v_land.at[turn, stage, half],
            r.v_sem.at[0, turn, stage, half],
            r.v_sem.at[1, turn, stage, half],
            tensor=2 * xor(chip, 1 << bit, bits) + core,
        )

    def grad_copy(turn, side):
        return remote(
            r.grad_v.at[turn, side],
            r.grad_v.at[turn, side],
            r.g_sem.at[0, turn],
            r.g_sem.at[1, turn],
            tensor=partner,
        )

    def misfit_start(turn):
        mark(f"za_misfit{turn}")
        r.m_send[turn] = r.part[turn, given].astype(bf16)
        misfit_copy(turn).start()

    def double_start(turn, stage):
        mark(f"zb_dstart{turn}{stage}")
        if stage == 0:
            misfit_copy(turn).wait_recv()
            total = r.part[turn, kept] + r.m_land[turn].astype(f32)
            values = [total[:, :half_cols], total[:, half_cols:]]
        else:
            values = doubled(turn, stage - 1)
        for half in range(2):
            r.v_share[turn, stage, half] = values[half].astype(bf16)
            double_copy(turn, stage, half).start()

    def doubled(turn, stage):
        values = []
        for half in range(2):
            double_copy(turn, stage, half).wait_recv()
            values.append(
                r.v_share[turn, stage, half].astype(f32)
                + r.v_land[turn, stage, half].astype(f32)
            )
        return values

    def grad_start(turn):
        mark(f"zc_gstart{turn}")
        values = doubled(turn, bits - 1)
        for half in range(2):
            span = slice(half * half_cols, (half + 1) * half_cols)
            r.grad_v[turn, core, :, span] = (values[half] * loss_scale).astype(bf16)
        grad_copy(turn, core).start()

    grad_hidden = Chain(r.gh, r.gh_land, r.gh_share, r.gh_sem.at[0], r.gh_sem.at[1], b, groups)

    def back(turn):
        mark(f"zd_back{turn}")
        grad_copy(turn, 1 - core).wait_recv()
        for side in range(2):
            first = turn * tall + side * short
            r.o_grad[first : first + short] = r.grad_v[turn, side]
        rows = slice(turn * tall, (turn + 1) * tall)
        for chunk in range(chunks):
            span = slice(chunk * cols, (chunk + 1) * cols)
            r.gh[turn * chunks + chunk] = jnp.dot(
                r.o_grad[rows], r.wd[:, span], preferred_element_type=f32
            )
        grad_hidden.origin(turn * chunks, (turn + 1) * chunks)

    def last(turn):
        mark(f"zf_elem{turn}")
        rows = slice(turn * tall, (turn + 1) * tall)
        for chunk in range(chunks):
            item = turn * chunks + chunk
            grad_hidden.total(item)
            span = slice(chunk * cols, (chunk + 1) * cols)
            gate, up, grad = r.gu[item, 0], r.gu[item, 1], r.gh[item]
            sigma = jax.nn.sigmoid(gate)
            r.o_gate[rows, span] = (
                grad * up * sigma * (1.0 + gate * (1.0 - sigma))
            ).astype(bf16)
            r.o_up[rows, span] = (grad * gate * sigma).astype(bf16)

    def steps(chain, *items):
        for late, item in items:
            mark(f"chain{'gh' if chain is grad_hidden else 'gu'}{late}{item}")
            chain.step(item, bool(late))

    def both(chain, first, final, skew):
        for step in range(first, final + skew):
            if step < final:
                steps(chain, (0, step))
            if step - skew >= first:
                steps(chain, (1, step - skew))

    items = 2 * chunks
    skew = 2
    order = []
    for step in range(items + skew):
        if step < items:
            order.append((0, step))
        if step >= skew:
            order.append((1, step - skew))
    ready = order.index((1, chunks - 1)) + 1

    steps(gate_up, *order[:1])
    target_home()
    steps(gate_up, *order[1:4])
    target_relay()
    steps(gate_up, *order[4 : ready - 3])
    target_end()
    steps(gate_up, *order[ready - 3 : ready])
    down(0)
    misfit_start(0)
    rest = order[ready:]
    per = -(-len(rest) // (bits + 1))
    for stage in range(bits):
        steps(gate_up, *rest[stage * per : (stage + 1) * per])
        double_start(0, stage)
    steps(gate_up, *rest[bits * per : -1])
    grad_start(0)
    steps(gate_up, *rest[-1:])
    down(1)
    misfit_start(1)
    back(0)
    double_start(1, 0)
    order = []
    for step in range(chunks + skew):
        if step < chunks:
            order.append((0, step))
        if step >= skew:
            order.append((1, step - skew))
    steps(grad_hidden, *order[:2])
    for stage in range(1, bits):
        double_start(1, stage)
    steps(grad_hidden, *order[2:3])
    grad_start(1)
    steps(grad_hidden, *order[3:4])
    back(1)
    mark("zg_full0")
    for stage in range(1, bits):
        full_sum.receive(stage - 1)
        full_sum.send(stage)
    steps(grad_hidden, *order[4:])
    last(0)
    both(grad_hidden, chunks, items, skew)
    last(1)

    mark("zg_full")
    full_sum.receive(bits - 1)
    for half in range(2):
        span = slice(half * (tokens // 2), (half + 1) * (tokens // 2))
        value = full_sum.final(half).T + r.resid_v[:, span].astype(f32)
        r.o_teacher[:, span] = value.astype(bf16)

    mark("zh_drain")
    for copy in x_copies:
        copy.wait_send()
    for step in range(1, groups):
        count_copy(step).wait_send()
    for relative in range(chips):
        for send, land, sem in (few[1:], many[1:], (r.c_send, r.c_land, r.c_sem)):
            pair_copy(send, land, sem, relative).wait_send()
        peer = xor(chip, relative, bits)
        wait_send_if(peer != b, z_copy(relative, peer))
    wait_send_if(jnp.logical_not(home_plane), target_z(chip))
    sq_copy.wait_send()
    row_copy.wait_send()
    for turn in range(2):
        misfit_copy(turn).wait_send()
        grad_copy(turn, core).wait_send()
        for stage in range(bits):
            for half in range(2):
                double_copy(turn, stage, half).wait_send()
    routed_sum.drain()
    target_sum.drain()
    full_sum.drain()
    gate_up.drain()
    grad_hidden.drain()
    mark(None)


def grads_kernel(rows, gate, up, grad, hidden, teacher, o_gate, o_up, o_down, o_teacher):
    o_gate[...] = contract(rows[...], gate[...], 0, 0)
    o_up[...] = contract(rows[...], up[...], 0, 0)
    o_down[...] = contract(grad[...], hidden[...], 0, 0)
    o_teacher[...] = teacher[...]


def on_device(
    attn_values,
    out_weight,
    residual_t,
    projector,
    student_input,
    norm_gain,
    w_gate,
    w_up,
    w_down,
    route_index,
):
    groups, tensors = lax.axis_size("batch"), lax.axis_size("tensor")
    chips = tensors // 2
    bits = chips.bit_length() - 1
    if chips != groups or 1 << bits != chips:
        raise ValueError("mesh")
    mean_routed = student_input.shape[0] // 8
    routed = mean_routed * groups
    tokens, heads = attn_values.shape
    feats = out_weight.shape[1] // tensors
    model = projector.shape[1]
    width = student_input.shape[1]
    block, units = w_gate.shape
    slots = route_index.shape[1]
    cols = min(256, units)
    chunks = units // cols
    dma = pltpu.SemaphoreType.DMA
    moved = chips - 1
    scratch = [
        pltpu.VMEM((slots + tokens, heads), bf16),
        pltpu.VMEM((tensors, heads, feats), bf16),
        pltpu.VMEM(residual_t.shape, bf16),
        pltpu.VMEM((tensors, feats, width), bf16),
        pltpu.VMEM(student_input.shape, bf16),
        pltpu.VMEM(w_gate.shape, bf16),
        pltpu.VMEM(w_up.shape, bf16),
        pltpu.VMEM(w_down.shape, bf16),
        dma((6 + 2 * tensors,)),
        pltpu.VMEM((chips, slots, feats), bf16),
        pltpu.VMEM((chips, slots, feats), bf16),
        dma((2, chips)),
        pltpu.VMEM((chips, tokens, feats), bf16),
        pltpu.VMEM((chips, tokens, feats), bf16),
        pltpu.VMEM((chips, 2, slots // 2, feats), bf16),
        pltpu.VMEM((moved, 2, slots // 2, feats), bf16),
        pltpu.VMEM((chips, 2, tokens // 2, feats), bf16),
        pltpu.VMEM((moved, 2, tokens // 2, feats), bf16),
        dma((2, chips)),
        dma((2, moved, 2)),
        dma((2, moved, 2)),
        pltpu.VMEM((chips, slots, width), bf16),
        pltpu.VMEM((chips, slots, width), bf16),
        pltpu.VMEM((chips, 2, slots // 2, width), bf16),
        pltpu.VMEM((moved, 2, slots // 2, width), bf16),
        pltpu.VMEM((slots, feats), bf16),
        pltpu.VMEM((slots, width), bf16),
        pltpu.VMEM((groups, slots, width), bf16),
        dma((2, chips)),
        dma((2, moved, 2)),
        dma((1 + groups,)),
        pltpu.VMEM((chips, slots, width), bf16),
        pltpu.VMEM((slots, 128), f32),
        pltpu.VMEM((slots, 128), f32),
        pltpu.VMEM((groups, 8, 128), f32),
        dma((2, chips)),
        dma((2,)),
        dma((2, groups)),
        pltpu.VMEM((chips, slots, width), bf16),
        pltpu.VMEM((groups, slots, width), bf16),
        dma((2, max(chips, groups))),
        pltpu.VMEM((groups, routed, slots), bf16),
        pltpu.VMEM((2, routed, width), bf16),
        dma((2,)),
        pltpu.VMEM((2 * chunks, 2, routed // 2, cols), f32),
        pltpu.VMEM((2, 2 * chunks, 2, routed // 2, cols), bf16),
        pltpu.VMEM((2, 2 * chunks, 2, routed // 2, cols), bf16),
        dma((2, 2, 2 * chunks)),
        pltpu.VMEM((2 * chunks, routed // 2, cols), f32),
        pltpu.VMEM((2, 2 * chunks, routed // 2, cols), bf16),
        pltpu.VMEM((2, 2 * chunks, routed // 2, cols), bf16),
        dma((2, 2, 2 * chunks)),
        pltpu.VMEM((2, routed // 2, block), f32),
        pltpu.VMEM((2, routed // 4, block), bf16),
        pltpu.VMEM((2, routed // 4, block), bf16),
        pltpu.VMEM((2, bits, 2, routed // 4, block // 2), bf16),
        pltpu.VMEM((2, bits, 2, routed // 4, block // 2), bf16),
        dma((2, 2)),
        dma((2, 2, bits, 2)),
        pltpu.VMEM((2, 2, routed // 4, block), bf16),
        dma((2, 2)),
    ]
    rows, gate, up, grad, hidden, teacher = pl.pallas_call(
        functools.partial(exchange_kernel, (groups, tensors, mean_routed)),
        name="exchange",
        out_shape=(
            jax.ShapeDtypeStruct((routed, block), bf16),
            jax.ShapeDtypeStruct((routed, units), bf16),
            jax.ShapeDtypeStruct((routed, units), bf16),
            jax.ShapeDtypeStruct((routed, block), bf16),
            jax.ShapeDtypeStruct((routed, units), bf16),
            jax.ShapeDtypeStruct(residual_t.shape, bf16),
        ),
        in_specs=[ANY, ANY, ANY, ANY, ANY, VMEM, ANY, ANY, ANY, VMEM],
        out_specs=[VMEM] * 6,
        scratch_shapes=scratch,
        compiler_params=pltpu.CompilerParams(
            collective_id=1, has_side_effects=True, vmem_limit_bytes=VMEM_BYTES
        ),
    )(
        attn_values,
        out_weight,
        residual_t,
        projector,
        student_input,
        norm_gain.reshape(1, -1),
        w_gate,
        w_up,
        w_down,
        route_index,
    )
    parts = 4
    tall = block // parts
    high = residual_t.shape[0] // parts
    whole = lambda array: pl.BlockSpec(array.shape, lambda i: (0, 0))
    strip = pl.BlockSpec((routed, tall), lambda i: (0, i))
    out = pl.BlockSpec((tall, units), lambda i: (i, 0))
    flat = pl.BlockSpec((high, residual_t.shape[1]), lambda i: (i, 0))
    grads = jax.ShapeDtypeStruct((block, units), f32)
    grad_gate, grad_up, grad_down, teacher_hidden = pl.pallas_call(
        grads_kernel,
        name="grads",
        grid=(parts,),
        out_shape=(grads, grads, grads, jax.ShapeDtypeStruct(residual_t.shape, bf16)),
        in_specs=[strip, whole(gate), whole(up), strip, whole(hidden), flat],
        out_specs=[out, out, out, flat],
    )(rows, gate, up, grad, hidden, teacher)
    return (teacher_hidden, grad_gate, grad_up, grad_down)


def solution(mesh):
    in_specs = (
        P("batch", "tensor"),
        P("tensor", None),
        P("tensor", "batch"),
        P("tensor", None),
        P("batch", "tensor"),
        P(),
        P("batch", "tensor"),
        P("batch", "tensor"),
        P("batch", "tensor"),
        P("batch", None),
    )
    out_specs = (
        P("tensor", "batch"),
        P("batch", "tensor"),
        P("batch", "tensor"),
        P("batch", "tensor"),
    )
    return jax.shard_map(
        on_device, mesh=mesh, in_specs=in_specs, out_specs=out_specs, check_vma=False
    )
```

```python
import functools
import math
import types

import jax
import jax.numpy as jnp
from jax import lax
from jax.experimental import pallas as pl
from jax.experimental.pallas import tpu as pltpu
from jax.sharding import PartitionSpec as P

epsilon = 1e-05
f32 = jnp.float32
bf16 = jnp.bfloat16
VMEM = pl.BlockSpec(memory_space=pltpu.VMEM)
HBM = pl.BlockSpec(memory_space=pltpu.HBM)
VMEM_BYTES = 54_000_000

NAMES = (
    "attn", "out_weight", "residual", "projector", "student", "gain", "w_gate", "w_up",
    "w_down", "route", "o_rows", "o_gate", "o_up", "o_grad", "o_hidden", "o_teacher",
    "attn_v", "weight_v", "resid_v", "proj_v", "stud_v", "wg", "wu", "wd", "route_v", "gain_v",
    "load_sem",
    "q_send", "q_land", "q_sem", "t_send", "t_land", "r_acc", "r_land", "f_acc", "f_land", "t_sem", "r_sem", "f_sem",
    "c_send", "c_land", "p_acc", "p_land", "p_keep", "p_send", "p_zland", "c_sem", "p_sem", "z2_sem",
    "x_land", "sq_send", "sq_land", "count_land", "x_sem", "sq_sem", "count_sem", "z_send",
    "z_land", "z_sem", "select", "rows_v", "row_sem", "gu", "gu_land", "gu_share", "gu_sem", "gh",
    "gh_land", "gh_share", "gh_sem", "part", "m_send", "m_land", "v_share", "v_land", "m_sem",
    "v_sem", "grad_v", "g_sem",
)
PROFILE = False
open_scope = []


def mark(name):
    if not PROFILE:
        return
    while open_scope:
        open_scope.pop().__exit__(None, None, None)
    if name:
        scope = jax.named_scope(name)
        scope.__enter__()
        open_scope.append(scope)


def contract(left, right, left_dim, right_dim):
    return lax.dot_general(
        left, right, (((left_dim,), (right_dim,)), ((), ())), preferred_element_type=f32
    )


def remote(src, dst, send_sem, recv_sem, **where):
    return pltpu.make_async_remote_copy(
        src_ref=src,
        dst_ref=dst,
        send_sem=send_sem,
        recv_sem=recv_sem,
        device_id=where,
        device_id_type=pl.DeviceIdType.MESH,
    )


def start_if(cond, copy):
    @pl.when(cond)
    def _():
        copy.start()


def wait_send_if(cond, copy):
    @pl.when(cond)
    def _():
        copy.wait_send()


def wait_recv_if(cond, copy):
    @pl.when(cond)
    def _():
        copy.wait_recv()


def xor(left, right, bits):
    total = 0
    for bit in range(bits):
        step = 1 << bit
        total = total + step * lax.rem(left // step + right // step, 2)
    return total


class Chain:
    def __init__(self, own, land, share, send_sem, recv_sem, me, size):
        self.own, self.land, self.share = own, land, share
        self.send_sem, self.recv_sem = send_sem, recv_sem
        self.me, self.size, self.chunks = me, size, own.shape[0]
        self.early = jnp.where(2 * me < size, 0, 1)

    def flow(self, late):
        way = 1 - self.early if late else self.early
        before = jnp.where(way == 0, self.me, self.size - 1 - self.me) > 0
        after = jnp.where(way == 0, self.size - 1 - self.me, self.me) > 0
        peer = jnp.where(way == 0, self.me + 1, self.me - 1)
        return way, before, after, peer

    def copy(self, way, chunk, peer):
        return remote(
            self.share.at[way, chunk],
            self.land.at[way, chunk],
            self.send_sem.at[way, chunk],
            self.recv_sem.at[way, chunk],
            batch=peer,
        )

    def origin(self, first, last):
        way, before, after, peer = self.flow(False)

        @pl.when(jnp.logical_not(before))
        def _():
            for chunk in range(first, last):
                self.share[way, chunk] = self.own[chunk].astype(bf16)
                self.copy(way, chunk, peer).start()

    def step(self, chunk, late):
        way, before, after, peer = self.flow(late)
        copy = self.copy(way, chunk, peer)

        @pl.when(jnp.logical_and(after, before))
        def _():
            copy.wait_recv()
            self.share[way, chunk] = (
                self.own[chunk] + self.land[way, chunk].astype(f32)
            ).astype(bf16)
            copy.start()

    def total(self, chunk):
        way, before, after, peer = self.flow(True)
        wait_recv_if(
            jnp.logical_and(before, jnp.logical_not(after)), self.copy(way, chunk, peer)
        )

        @pl.when(self.me > 0)
        def _():
            self.own[chunk] = self.own[chunk] + self.land[0, chunk].astype(f32)

        @pl.when(self.me < self.size - 1)
        def _():
            self.own[chunk] = self.own[chunk] + self.land[1, chunk].astype(f32)

    def drain(self):
        for late in (False, True):
            way, _, after, peer = self.flow(late)
            for chunk in range(self.chunks):
                wait_send_if(after, self.copy(way, chunk, peer))


class PlaneScatter:
    def __init__(self, acc, land, send_sem, recv_sem, chip, core, bits, absolute=False):
        self.acc, self.land, self.absolute = acc, land, absolute
        self.send_sem, self.recv_sem = send_sem, recv_sem
        self.chip, self.core, self.bits = chip, core, bits
        self.slots, self.stages = [], []
        for half in range(2):
            order = [1 << bit for bit in range(bits)]
            order = order if half == 0 else order[::-1]
            used, slots, stages = 0, {}, []
            done = 0
            for stage, flip in enumerate(order):
                moved = [
                    block
                    for block in range((1 << bits) - 1, -1, -1)
                    if block & flip and not block & done
                ]
                for block in moved:
                    slots[(stage, block ^ flip)] = used
                    used += 1
                stages.append((flip, moved))
                done |= flip
            self.slots.append(slots)
            self.stages.append(stages)

    def place(self, block):
        return xor(self.chip, block, self.bits) if self.absolute else block

    def copy(self, half, stage, block):
        flip, _ = self.stages[half][stage]
        slot = self.slots[half][(stage, block ^ flip)]
        return remote(
            self.acc.at[self.place(block), half],
            self.land.at[slot, half],
            self.send_sem.at[slot, half],
            self.recv_sem.at[slot, half],
            tensor=2 * xor(self.chip, flip, self.bits) + self.core,
        )

    def arrived(self, half, stages, block):
        return [
            self.land[self.slots[half][(stage, block)], half].astype(f32)
            for stage in range(stages)
        ]

    def send(self, stage, first=0, last=None):
        for half in range(2):
            for block in self.stages[half][stage][1][first:last]:
                place = self.place(block)
                if stage:
                    value = self.acc[place, half].astype(f32)
                    for term in self.arrived(half, stage, block):
                        value = value + term
                    self.acc[place, half] = value.astype(bf16)
                self.copy(half, stage, block).start()

    def receive(self, stage):
        for half in range(2):
            for block in self.stages[half][stage][1]:
                self.copy(half, stage, block).wait_recv()

    def final(self, half):
        value = self.acc[self.place(0), half].astype(f32)
        for term in self.arrived(half, self.bits, 0):
            value = value + term
        return value

    def drain(self):
        for half in range(2):
            for stage in range(self.bits):
                for block in self.stages[half][stage][1]:
                    self.copy(half, stage, block).wait_send()


def exchange_kernel(dims, *refs):
    (groups, tensors, mean_routed) = dims
    r = types.SimpleNamespace(**dict(zip(NAMES, refs, strict=True)))

    b, t = lax.axis_index("batch"), lax.axis_index("tensor")
    chips = tensors // 2
    bits = chips.bit_length() - 1
    chip, core = t // 2, lax.rem(t, 2)
    partner = t + 1 - 2 * core
    slots = r.route.shape[1]
    tokens, heads = r.attn.shape
    feats = r.out_weight.shape[1] // tensors
    width = r.student.shape[1]
    block = r.w_gate.shape[0]
    hidden_units = r.w_gate.shape[1]
    routed = mean_routed * groups
    tall = routed // 2
    short = routed // 4
    chunks = r.gu.shape[0] // 2
    cols = hidden_units // chunks
    portion = slots // chips
    others = range(1, chips)

    mark("a_loads")
    loads = {}

    def load(name, src, dst):
        copy = pltpu.make_async_copy(src, dst, r.load_sem.at[len(loads)])
        copy.start()
        loads[name] = copy

    def weight_block(index):
        place = pl.multiple_of(index * feats, feats)
        return r.out_weight.at[:, pl.ds(place, feats)]

    def owner(relative, side):
        return 2 * xor(chip, relative, bits) + (core if side else 1 - core)

    load("route", r.route, r.route_v)
    load("student", r.student, r.stud_v)
    load("attn", r.attn, r.attn_v.at[pl.ds(slots, tokens)])
    for side in range(2):
        for step in range(chips):
            place = side * chips + step
            index = owner(chips - 1 - step, side)
            load(("w", place), weight_block(index), r.weight_v.at[place])
    load("gain", r.gain, r.gain_v)
    load("w_gate", r.w_gate, r.wg)
    load("w_up", r.w_up, r.wu)
    load("residual", r.residual, r.resid_v)
    for side in range(2):
        for step in range(chips):
            index = 2 * step + (core if side else 1 - core)
            place = pl.multiple_of(index * width, width)
            load(
                ("p", side * chips + step),
                r.projector.at[:, pl.ds(place, width)],
                r.proj_v.at[side * chips + step],
            )
    load("w_down", r.w_down, r.wd)

    barrier = pltpu.get_barrier_semaphore()
    for step in others:
        pl.semaphore_signal(
            barrier,
            inc=1,
            device_id={"tensor": 2 * xor(chip, step, bits) + core},
            device_id_type=pl.DeviceIdType.MESH,
        )
    pl.semaphore_signal(
        barrier, inc=1, device_id={"tensor": partner}, device_id_type=pl.DeviceIdType.MESH
    )
    for step in range(1, groups):
        pl.semaphore_signal(
            barrier,
            inc=1,
            device_id={"batch": lax.rem(b + step, groups)},
            device_id_type=pl.DeviceIdType.MESH,
        )

    mark("b_route")
    loads["route"].wait()
    route = r.route_v[...]
    row_id = lax.broadcasted_iota(jnp.int32, (slots, slots), 0)
    col_id = lax.broadcasted_iota(jnp.int32, (slots, slots), 1)
    route_col = jnp.sum(jnp.where(row_id == col_id, route, 0), axis=1, keepdims=True)
    token_id = lax.broadcasted_iota(jnp.int32, (slots, tokens), 1)
    pick = jnp.where(token_id == route_col, 1.0, 0.0).astype(bf16)
    count = jnp.sum(jnp.where(route >= 0, 1.0, 0.0), axis=1, keepdims=True)
    r.count_land[b] = jnp.broadcast_to(count, r.count_land.shape[1:])

    loads["student"].wait()
    r.x_land[0] = contract(pick, r.stud_v[...], 1, 0).astype(bf16)

    mark("c_barrier")
    pl.semaphore_wait(barrier, chips - 1 + 1 + groups - 1)

    mark("d_tprep")
    x_copies = [
        remote(
            r.x_land.at[0],
            r.x_land.at[step],
            r.x_sem.at[0, step],
            r.x_sem.at[1, step],
            tensor=2 * xor(chip, step, bits) + core,
        )
        for step in others
    ]
    for copy in x_copies[::-1]:
        copy.start()

    def count_copy(step):
        return remote(
            r.count_land.at[b],
            r.count_land.at[b],
            r.count_sem.at[0, step],
            r.count_sem.at[1, b],
            batch=lax.rem(b + step, groups),
        )

    for step in range(1, groups):
        count_copy(step).start()

    loads["attn"].wait()
    all_rows = slice(slots, slots + tokens)
    r.attn_v[0:slots] = contract(pick, r.attn_v[all_rows], 1, 0).astype(bf16)

    def pair_copy(send, land, sem, relative):
        return remote(
            send.at[relative],
            land.at[relative],
            sem.at[0, relative],
            sem.at[1, relative],
            tensor=partner,
        )

    piece = min(256, feats)

    def away(rows, send, land, sem, step):
        for place in range(0, feats, piece):
            span = slice(place, place + piece)
            value = jnp.dot(
                r.attn_v[rows], r.weight_v[step, :, span], preferred_element_type=f32
            )
            send[chips - 1 - step, :, span] = value.astype(bf16)
        pair_copy(send, land, sem, chips - 1 - step).start()

    def home(rows, send, land, sem, acc, step):
        relative = chips - 1 - step
        count = acc.shape[2]
        pair_copy(send, land, sem, relative).wait_recv()
        for place in range(0, feats, piece):
            span = slice(place, place + piece)
            value = jnp.dot(
                r.attn_v[rows], r.weight_v[chips + step, :, span], preferred_element_type=f32
            )
            value = (value + land[relative, :, span].astype(f32)).astype(bf16)
            for half in range(2):
                acc[relative, half, :, span] = value[half * count : (half + 1) * count]

    few = (slice(0, slots), r.q_send, r.q_land, r.q_sem)
    many = (all_rows, r.t_send, r.t_land, r.t_sem)
    routed_sum = PlaneScatter(
        r.r_acc, r.r_land, r.r_sem.at[0], r.r_sem.at[1], chip, core, bits
    )
    full_sum = PlaneScatter(
        r.f_acc, r.f_land, r.f_sem.at[0], r.f_sem.at[1], chip, core, bits
    )
    mark("e_away")
    for step in range(chips):
        loads[("w", step)].wait()
        away(*few, step)
    for step in range(chips):
        loads[("w", chips + step)].wait()
        home(*few, r.r_acc, step)
    routed_sum.send(0)

    mark("f_waitx")
    for copy in x_copies:
        copy.wait_recv()
    square = jnp.zeros((slots, 1), f32)
    for step in range(chips):
        value = r.x_land[step].astype(f32)
        square = square + jnp.sum(value * value, axis=1, keepdims=True)
    r.sq_send[...] = jnp.broadcast_to(square, r.sq_send.shape)
    sq_copy = remote(
        r.sq_send, r.sq_land, r.sq_sem.at[0], r.sq_sem.at[1], tensor=partner
    )
    sq_copy.start()
    away(*many, 0)
    mark("h_norm")
    sq_copy.wait_recv()
    square = r.sq_send[:, 0:1] + r.sq_land[:, 0:1]
    loads["gain"].wait()
    scale = lax.rsqrt(square / (width * tensors) + epsilon)

    def z_copy(relative, peer):
        return remote(
            r.z_send.at[relative],
            r.z_land.at[b],
            r.z_sem.at[0, relative],
            r.z_sem.at[1, b],
            batch=peer,
        )

    for relative in range(chips):
        peer = xor(chip, relative, bits)
        place = pl.multiple_of(peer * block + core * width, width)
        value = r.x_land[relative].astype(f32) * scale * r.gain_v[:, pl.ds(place, width)]
        value = value.astype(bf16)

        @pl.when(peer == b)
        def _():
            r.z_land[b] = value

        @pl.when(peer != b)
        def _():
            r.z_send[relative] = value
            z_copy(relative, peer).start()

    mark("i_home")
    for step in range(1, chips):
        away(*many, step)
    home(*many, r.f_acc, 0)
    mark("j_rrecv")
    routed_sum.receive(0)
    routed_sum.send(1)
    for stage in range(2, bits):
        routed_sum.receive(stage - 1)
        routed_sum.send(stage)
    full_sum.send(0, 0, 1)
    mark("j2_home")
    for step in range(1, chips):
        home(*many, r.f_acc, step)

    mark("k_waitz")
    for group in range(groups):
        for land, sem in ((r.count_land, r.count_sem), (r.z_land, r.z_sem)):
            wait_recv_if(
                group != b,
                remote(
                    land.at[group], land.at[group], sem.at[0, 0], sem.at[1, group], batch=b
                ),
            )
    mark("l_pack")
    pack_row = lax.broadcasted_iota(jnp.int32, (routed, slots), 0).astype(f32)
    pack_col = lax.broadcasted_iota(jnp.int32, (routed, slots), 1).astype(f32)
    mine_row = lax.broadcasted_iota(jnp.int32, (routed, portion), 0).astype(f32)
    mine_col = lax.broadcasted_iota(jnp.int32, (routed, portion), 1) + chip * portion
    mine_col = mine_col.astype(f32)
    offset = jnp.zeros((1, 1), f32)
    packed = jnp.zeros((routed, width), f32)
    for group in range(groups):
        amount = r.count_land[group][0:1, 0:1]
        hit = jnp.logical_and(pack_col + offset == pack_row, pack_col < amount)
        packed = packed + contract(jnp.where(hit, 1.0, 0.0).astype(bf16), r.z_land[group], 1, 0)
        hit = jnp.logical_and(mine_col + offset == mine_row, mine_col < amount)
        r.select[group] = jnp.where(hit, 1.0, 0.0).astype(bf16)
        offset = offset + amount
    r.rows_v[core] = packed.astype(bf16)
    row_copy = remote(
        r.rows_v.at[core], r.rows_v.at[core], r.row_sem.at[0], r.row_sem.at[1], tensor=partner
    )
    row_copy.start()

    mark("m_proj1")
    loads["w_gate"].wait()
    loads["w_up"].wait()

    def project(side, first):
        start = pl.multiple_of(side * width, width)
        rows = r.rows_v[side]
        for chunk in range(chunks):
            span = slice(chunk * cols, (chunk + 1) * cols)
            for which, weight in enumerate((r.wg, r.wu)):
                value = jnp.dot(
                    rows, weight[pl.ds(start, width), span], preferred_element_type=f32
                )
                for turn in range(2):
                    item = turn * chunks + chunk
                    piece = value[turn * tall : (turn + 1) * tall]
                    r.gu[item, which] = piece if first else r.gu[item, which] + piece

    project(core, True)
    mark("o_rowwait")
    remote(
        r.rows_v.at[1 - core],
        r.rows_v.at[1 - core],
        r.row_sem.at[0],
        r.row_sem.at[1],
        tensor=partner,
    ).wait_recv()
    mark("p_proj2")
    project(1 - core, False)
    gate_up = Chain(r.gu, r.gu_land, r.gu_share, r.gu_sem.at[0], r.gu_sem.at[1], b, groups)
    gate_up.origin(0, chunks)
    for side in range(2):
        r.o_rows[:, side * width : (side + 1) * width] = r.rows_v[side]

    mark("r_rrecv1")
    routed_sum.receive(bits - 1)
    loads["residual"].wait()
    routed_resid = contract(pick, r.resid_v[...], 1, 1)
    for half in range(2):
        first = half * (slots // 2)
        value = routed_sum.final(half) + routed_resid[first : first + slots // 2]
        r.p_keep[first : first + slots // 2] = value.astype(bf16)

    def target_copy(relative):
        return pair_copy(r.c_send, r.c_land, r.c_sem, relative)

    mark("s_target")
    for step in range(groups):
        loads[("p", step)].wait()
        value = jnp.dot(r.p_keep[...], r.proj_v[step], preferred_element_type=f32)
        r.c_send[step] = value.astype(bf16)
        target_copy(step).start()
    target_sum = PlaneScatter(
        r.p_acc, r.p_land, r.p_sem.at[0], r.p_sem.at[1], chip, core, bits, absolute=True
    )
    side_blocks = groups // 2

    def target_home():
        mark("u_target2")
        for step in range(groups):
            loads[("p", groups + step)].wait()
            value = jnp.dot(r.p_keep[...], r.proj_v[groups + step], preferred_element_type=f32)
            target_copy(step).wait_recv()
            value = (value + r.c_land[step].astype(f32)).astype(bf16)
            half, place = step // side_blocks, step % side_blocks * width
            for owner in range(chips):
                rows = value[owner * portion : (owner + 1) * portion]
                r.p_acc[owner, half, :, place : place + width] = rows
        target_sum.send(0)

    def target_relay():
        mark("v_trelay")
        for stage in range(1, bits):
            target_sum.receive(stage - 1)
            target_sum.send(stage)

    def target_z(peer):
        return remote(
            r.p_send.at[peer],
            r.p_zland.at[b],
            r.z2_sem.at[0, peer],
            r.z2_sem.at[1, b],
            batch=peer,
        )

    def target_end():
        mark("x_tz")
        target_sum.receive(bits - 1)
        for half in range(2):
            value = target_sum.final(half).astype(bf16)
            for place in range(side_blocks):
                peer = half * side_blocks + place
                part = value[:, place * width : (place + 1) * width]

                @pl.when(peer == b)
                def _():
                    r.p_zland[b] = part

                @pl.when(peer != b)
                def _():
                    r.p_send[peer] = part
                    target_z(peer).start()

        full_sum.send(0, 1)

    def down(turn):
        mark(f"y_down{turn}")
        rows = slice(turn * tall, (turn + 1) * tall)
        if turn == 0:
            loads["w_down"].wait()
        for chunk in range(chunks):
            item = turn * chunks + chunk
            gate_up.total(item)
            gate, up = r.gu[item, 0], r.gu[item, 1]
            value = (gate * jax.nn.sigmoid(gate) * up).astype(bf16)
            r.o_hidden[rows, chunk * cols : (chunk + 1) * cols] = value
        r.part[turn] = contract(r.o_hidden[rows], r.wd[...], 1, 1)

        mark(f"z_tarrive{turn}")
        value = jnp.zeros((tall, width), f32)
        for group in range(groups):
            if turn == 0:
                wait_recv_if(
                    group != b,
                    remote(
                        r.p_zland.at[group],
                        r.p_zland.at[group],
                        r.z2_sem.at[0, 0],
                        r.z2_sem.at[1, group],
                        batch=b,
                    ),
                )
            value = value + contract(r.select[group, rows], r.p_zland[group], 1, 0)
        span = pl.ds(pl.multiple_of(core * width, width), width)
        r.part[turn, :, span] = r.part[turn, :, span] - value

    kept = pl.ds(pl.multiple_of(core * short, short), short)
    given = pl.ds(pl.multiple_of((1 - core) * short, short), short)
    half_cols = block // 2
    loss_scale = 1.0 / math.sqrt(routed)

    def misfit_copy(turn):
        return remote(
            r.m_send.at[turn],
            r.m_land.at[turn],
            r.m_sem.at[0, turn],
            r.m_sem.at[1, turn],
            tensor=partner,
        )

    def double_copy(turn, stage, half):
        bit = stage if half == 0 else bits - 1 - stage
        return remote(
            r.v_share.at[turn, stage, half],
            r.v_land.at[turn, stage, half],
            r.v_sem.at[0, turn, stage, half],
            r.v_sem.at[1, turn, stage, half],
            tensor=2 * xor(chip, 1 << bit, bits) + core,
        )

    def grad_copy(turn, side):
        return remote(
            r.grad_v.at[turn, side],
            r.grad_v.at[turn, side],
            r.g_sem.at[0, turn],
            r.g_sem.at[1, turn],
            tensor=partner,
        )

    def misfit_start(turn):
        mark(f"za_misfit{turn}")
        r.m_send[turn] = r.part[turn, given].astype(bf16)
        misfit_copy(turn).start()

    def double_start(turn, stage):
        mark(f"zb_dstart{turn}{stage}")
        if stage == 0:
            misfit_copy(turn).wait_recv()
            total = r.part[turn, kept] + r.m_land[turn].astype(f32)
            values = [total[:, :half_cols], total[:, half_cols:]]
        else:
            values = doubled(turn, stage - 1)
        for half in range(2):
            r.v_share[turn, stage, half] = values[half].astype(bf16)
            double_copy(turn, stage, half).start()

    def doubled(turn, stage):
        values = []
        for half in range(2):
            double_copy(turn, stage, half).wait_recv()
            values.append(
                r.v_share[turn, stage, half].astype(f32)
                + r.v_land[turn, stage, half].astype(f32)
            )
        return values

    def grad_start(turn):
        mark(f"zc_gstart{turn}")
        values = doubled(turn, bits - 1)
        for half in range(2):
            span = slice(half * half_cols, (half + 1) * half_cols)
            r.grad_v[turn, core, :, span] = (values[half] * loss_scale).astype(bf16)
        grad_copy(turn, core).start()

    grad_hidden = Chain(r.gh, r.gh_land, r.gh_share, r.gh_sem.at[0], r.gh_sem.at[1], b, groups)

    def back(turn):
        mark(f"zd_back{turn}")
        grad_copy(turn, 1 - core).wait_recv()
        for side in range(2):
            first = turn * tall + side * short
            r.o_grad[first : first + short] = r.grad_v[turn, side]
        rows = slice(turn * tall, (turn + 1) * tall)
        for chunk in range(chunks):
            span = slice(chunk * cols, (chunk + 1) * cols)
            r.gh[turn * chunks + chunk] = jnp.dot(
                r.o_grad[rows], r.wd[:, span], preferred_element_type=f32
            )
        grad_hidden.origin(turn * chunks, (turn + 1) * chunks)

    def last(turn):
        mark(f"zf_elem{turn}")
        rows = slice(turn * tall, (turn + 1) * tall)
        for chunk in range(chunks):
            item = turn * chunks + chunk
            grad_hidden.total(item)
            span = slice(chunk * cols, (chunk + 1) * cols)
            gate, up, grad = r.gu[item, 0], r.gu[item, 1], r.gh[item]
            sigma = jax.nn.sigmoid(gate)
            r.o_gate[rows, span] = (
                grad * up * sigma * (1.0 + gate * (1.0 - sigma))
            ).astype(bf16)
            r.o_up[rows, span] = (grad * gate * sigma).astype(bf16)

    def steps(chain, *items):
        for late, item in items:
            mark(f"chain{'gh' if chain is grad_hidden else 'gu'}{late}{item}")
            chain.step(item, bool(late))

    def order_of(first, final, skew):
        order = []
        for step in range(first, final + skew):
            if step < final:
                order.append((0, step))
            if step - skew >= first:
                order.append((1, step - skew))
        return order

    items = 2 * chunks
    order = order_of(0, items, min(5, chunks))
    late = [order.index((1, item)) + 1 for item in range(items)]

    target_home()
    gate_up.origin(chunks, items)
    steps(gate_up, *order[: late[0] - 3])
    target_relay()
    steps(gate_up, *order[late[0] - 3 : late[chunks - 3]])
    target_end()
    begin = min(items - 2, chunks + 1)
    steps(gate_up, *order[late[chunks - 3] : late[begin]])
    down(0)
    misfit_start(0)
    for stage in range(bits):
        end = min(items - 1, begin + 2)
        steps(gate_up, *order[late[begin] : late[end]])
        double_start(0, stage)
        begin = end
    steps(gate_up, *order[late[begin] :])
    down(1)
    misfit_start(1)
    grad_start(0)
    double_start(1, 0)
    back(0)

    order = order_of(0, chunks, chunks)
    late = [order.index((1, item)) + 1 for item in range(chunks)]
    steps(grad_hidden, *order[:2])
    for stage in range(1, bits):
        double_start(1, stage)
    steps(grad_hidden, *order[2 : late[0] - 1])
    grad_start(1)
    steps(grad_hidden, *order[late[0] - 1 : late[3]])
    back(1)
    mark("zg_full0")
    for stage in range(1, bits):
        full_sum.receive(stage - 1)
        full_sum.send(stage)
    steps(grad_hidden, *order[late[3] :])
    last(0)
    steps(grad_hidden, *order_of(chunks, items, chunks))
    last(1)

    mark("zg_full")
    full_sum.receive(bits - 1)
    for half in range(2):
        span = slice(half * (tokens // 2), (half + 1) * (tokens // 2))
        value = full_sum.final(half).T + r.resid_v[:, span].astype(f32)
        r.o_teacher[:, span] = value.astype(bf16)

    mark("zh_drain")
    for copy in x_copies:
        copy.wait_send()
    for step in range(1, groups):
        count_copy(step).wait_send()
    for relative in range(chips):
        for send, land, sem in (few[1:], many[1:], (r.c_send, r.c_land, r.c_sem)):
            pair_copy(send, land, sem, relative).wait_send()
        peer = xor(chip, relative, bits)
        wait_send_if(peer != b, z_copy(relative, peer))
    for peer in range(groups):
        wait_send_if(peer != b, target_z(peer))
    sq_copy.wait_send()
    row_copy.wait_send()
    for turn in range(2):
        misfit_copy(turn).wait_send()
        grad_copy(turn, core).wait_send()
        for stage in range(bits):
            for half in range(2):
                double_copy(turn, stage, half).wait_send()
    routed_sum.drain()
    target_sum.drain()
    full_sum.drain()
    gate_up.drain()
    grad_hidden.drain()
    mark(None)


def grads_kernel(
    rows, gate, up, grad, hidden, teacher, o_gate, o_up, o_down, o_teacher, hold, sem, end_sem
):
    count, parts, tall, _ = hold.shape
    copies = [pltpu.make_async_copy(teacher, o_teacher, end_sem.at[0])]
    copies[0].start()
    terms = ((grad, hidden, o_down), (rows, gate, o_gate), (rows, up, o_up))
    for which, (left, right, out) in enumerate(terms):
        for part in range(parts):
            span = pl.ds(part * tall, tall)
            hold[which, part] = contract(left[:, span], right[...], 0, 0)
            copy = pltpu.make_async_copy(hold.at[which, part], out.at[span], sem.at[which, part])
            copy.start()
            copies.append(copy)
    for copy in copies:
        copy.wait()


def on_device(
    attn_values,
    out_weight,
    residual_t,
    projector,
    student_input,
    norm_gain,
    w_gate,
    w_up,
    w_down,
    route_index,
):
    groups, tensors = lax.axis_size("batch"), lax.axis_size("tensor")
    chips = tensors // 2
    bits = chips.bit_length() - 1
    if chips != groups or 1 << bits != chips:
        raise ValueError("mesh")
    mean_routed = student_input.shape[0] // 8
    routed = mean_routed * groups
    tokens, heads = attn_values.shape
    feats = out_weight.shape[1] // tensors
    model = projector.shape[1]
    width = student_input.shape[1]
    block, units = w_gate.shape
    slots = route_index.shape[1]
    cols = min(128, units)
    chunks = units // cols
    dma = pltpu.SemaphoreType.DMA
    moved = chips - 1
    scratch = [
        pltpu.VMEM((slots + tokens, heads), bf16),
        pltpu.VMEM((tensors, heads, feats), bf16),
        pltpu.VMEM(residual_t.shape, bf16),
        pltpu.VMEM((tensors, feats, width), bf16),
        pltpu.VMEM(student_input.shape, bf16),
        pltpu.VMEM(w_gate.shape, bf16),
        pltpu.VMEM(w_up.shape, bf16),
        pltpu.VMEM(w_down.shape, bf16),
        pltpu.VMEM(route_index.shape, route_index.dtype),
        pltpu.VMEM((1, model), f32),
        dma((8 + 2 * tensors,)),
        pltpu.VMEM((chips, slots, feats), bf16),
        pltpu.VMEM((chips, slots, feats), bf16),
        dma((2, chips)),
        pltpu.VMEM((chips, tokens, feats), bf16),
        pltpu.VMEM((chips, tokens, feats), bf16),
        pltpu.VMEM((chips, 2, slots // 2, feats), bf16),
        pltpu.VMEM((moved, 2, slots // 2, feats), bf16),
        pltpu.VMEM((chips, 2, tokens // 2, feats), bf16),
        pltpu.VMEM((moved, 2, tokens // 2, feats), bf16),
        dma((2, chips)),
        dma((2, moved, 2)),
        dma((2, moved, 2)),
        pltpu.VMEM((chips, slots, width), bf16),
        pltpu.VMEM((chips, slots, width), bf16),
        pltpu.VMEM((chips, 2, slots // chips, model // 4), bf16),
        pltpu.VMEM((moved, 2, slots // chips, model // 4), bf16),
        pltpu.VMEM((slots, feats), bf16),
        pltpu.VMEM((groups, slots // chips, width), bf16),
        pltpu.VMEM((groups, slots // chips, width), bf16),
        dma((2, chips)),
        dma((2, moved, 2)),
        dma((2, groups)),
        pltpu.VMEM((chips, slots, width), bf16),
        pltpu.VMEM((slots, 128), f32),
        pltpu.VMEM((slots, 128), f32),
        pltpu.VMEM((groups, 8, 128), f32),
        dma((2, chips)),
        dma((2,)),
        dma((2, groups)),
        pltpu.VMEM((chips, slots, width), bf16),
        pltpu.VMEM((groups, slots, width), bf16),
        dma((2, max(chips, groups))),
        pltpu.VMEM((groups, routed, slots // chips), bf16),
        pltpu.VMEM((2, routed, width), bf16),
        dma((2,)),
        pltpu.VMEM((2 * chunks, 2, routed // 2, cols), f32),
        pltpu.VMEM((2, 2 * chunks, 2, routed // 2, cols), bf16),
        pltpu.VMEM((2, 2 * chunks, 2, routed // 2, cols), bf16),
        dma((2, 2, 2 * chunks)),
        pltpu.VMEM((2 * chunks, routed // 2, cols), f32),
        pltpu.VMEM((2, 2 * chunks, routed // 2, cols), bf16),
        pltpu.VMEM((2, 2 * chunks, routed // 2, cols), bf16),
        dma((2, 2, 2 * chunks)),
        pltpu.VMEM((2, routed // 2, block), f32),
        pltpu.VMEM((2, routed // 4, block), bf16),
        pltpu.VMEM((2, routed // 4, block), bf16),
        pltpu.VMEM((2, bits, 2, routed // 4, block // 2), bf16),
        pltpu.VMEM((2, bits, 2, routed // 4, block // 2), bf16),
        dma((2, 2)),
        dma((2, 2, bits, 2)),
        pltpu.VMEM((2, 2, routed // 4, block), bf16),
        dma((2, 2)),
    ]
    rows, gate, up, grad, hidden, teacher = pl.pallas_call(
        functools.partial(exchange_kernel, (groups, tensors, mean_routed)),
        name="exchange",
        out_shape=(
            jax.ShapeDtypeStruct((routed, block), bf16),
            jax.ShapeDtypeStruct((routed, units), bf16),
            jax.ShapeDtypeStruct((routed, units), bf16),
            jax.ShapeDtypeStruct((routed, block), bf16),
            jax.ShapeDtypeStruct((routed, units), bf16),
            jax.ShapeDtypeStruct(residual_t.shape, bf16),
        ),
        in_specs=[HBM] * 10,
        out_specs=[VMEM] * 6,
        scratch_shapes=scratch,
        compiler_params=pltpu.CompilerParams(
            collective_id=1, has_side_effects=True, vmem_limit_bytes=VMEM_BYTES
        ),
    )(
        attn_values,
        out_weight,
        residual_t,
        projector,
        student_input,
        norm_gain.reshape(1, -1),
        w_gate,
        w_up,
        w_down,
        route_index,
    )
    parts = 4
    grads = jax.ShapeDtypeStruct((block, units), f32)
    grad_gate, grad_up, grad_down, teacher_hidden = pl.pallas_call(
        grads_kernel,
        name="grads",
        out_shape=(grads, grads, grads, jax.ShapeDtypeStruct(residual_t.shape, bf16)),
        in_specs=[VMEM] * 6,
        out_specs=[HBM] * 4,
        scratch_shapes=[
            pltpu.VMEM((3, parts, block // parts, units), f32),
            dma((3, parts)),
            dma((1,)),
        ],
        compiler_params=pltpu.CompilerParams(vmem_limit_bytes=20_000_000),
    )(rows, gate, up, grad, hidden, teacher)
    return (teacher_hidden, grad_gate, grad_up, grad_down)


def solution(mesh):
    in_specs = (
        P("batch", "tensor"),
        P("tensor", None),
        P("tensor", "batch"),
        P("tensor", None),
        P("batch", "tensor"),
        P(),
        P("batch", "tensor"),
        P("batch", "tensor"),
        P("batch", "tensor"),
        P("batch", None),
    )
    out_specs = (
        P("tensor", "batch"),
        P("batch", "tensor"),
        P("batch", "tensor"),
        P("batch", "tensor"),
    )
    return jax.shard_map(
        on_device, mesh=mesh, in_specs=in_specs, out_specs=out_specs, check_vma=False
    )
```

```python
import functools
import math
import types

import jax
import jax.numpy as jnp
from jax import lax
from jax.experimental import pallas as pl
from jax.experimental.pallas import tpu as pltpu
from jax.sharding import PartitionSpec as P

epsilon = 1e-05
f32 = jnp.float32
bf16 = jnp.bfloat16
VMEM = pl.BlockSpec(memory_space=pltpu.VMEM)
HBM = pl.BlockSpec(memory_space=pltpu.HBM)
VMEM_BYTES = 54_000_000

NAMES = (
    "attn", "out_weight", "residual", "projector", "student", "gain", "w_gate", "w_up",
    "w_down", "route", "o_rows", "o_gate", "o_up", "o_grad", "o_hidden", "o_teacher",
    "attn_v", "weight_v", "resid_v", "proj_v", "stud_v", "wg", "wu", "wd", "route_v", "gain_v",
    "load_sem", "out_sem",
    "q_send", "q_land", "q_sem", "t_send", "t_land", "r_acc", "r_land", "f_acc", "f_land", "t_sem", "r_sem", "f_sem",
    "c_send", "c_land", "p_acc", "p_land", "p_keep", "p_send", "p_zland", "c_sem", "p_sem", "z2_sem",
    "x_land", "sq_send", "sq_land", "count_land", "x_sem", "sq_sem", "count_sem", "z_send",
    "z_land", "z_sem", "select", "rows_v", "row_sem", "gu", "gu_land", "gu_share", "gu_sem", "gh",
    "gh_land", "gh_share", "gh_sem", "part", "m_send", "m_land", "v_share", "v_land", "m_sem",
    "v_sem", "grad_v", "g_sem",
)


def contract(left, right, left_dim, right_dim):
    return lax.dot_general(
        left, right, (((left_dim,), (right_dim,)), ((), ())), preferred_element_type=f32
    )


def remote(src, dst, send_sem, recv_sem, **where):
    return pltpu.make_async_remote_copy(
        src_ref=src,
        dst_ref=dst,
        send_sem=send_sem,
        recv_sem=recv_sem,
        device_id=where,
        device_id_type=pl.DeviceIdType.MESH,
    )


def start_if(cond, copy):
    @pl.when(cond)
    def _():
        copy.start()


def wait_send_if(cond, copy):
    @pl.when(cond)
    def _():
        copy.wait_send()


def wait_recv_if(cond, copy):
    @pl.when(cond)
    def _():
        copy.wait_recv()


def xor(left, right, bits):
    total = 0
    for bit in range(bits):
        step = 1 << bit
        total = total + step * lax.rem(left // step + right // step, 2)
    return total


class Chain:
    def __init__(self, own, land, share, send_sem, recv_sem, me, size):
        self.own, self.land, self.share = own, land, share
        self.send_sem, self.recv_sem = send_sem, recv_sem
        self.me, self.size, self.chunks = me, size, own.shape[0]
        self.early = jnp.where(2 * me < size, 0, 1)

    def flow(self, late):
        way = 1 - self.early if late else self.early
        before = jnp.where(way == 0, self.me, self.size - 1 - self.me) > 0
        after = jnp.where(way == 0, self.size - 1 - self.me, self.me) > 0
        peer = jnp.where(way == 0, self.me + 1, self.me - 1)
        return way, before, after, peer

    def copy(self, way, chunk, peer):
        return remote(
            self.share.at[way, chunk],
            self.land.at[way, chunk],
            self.send_sem.at[way],
            self.recv_sem.at[way, chunk],
            batch=peer,
        )

    def origin(self, first, last):
        way, before, after, peer = self.flow(False)

        @pl.when(jnp.logical_not(before))
        def _():
            for chunk in range(first, last):
                self.share[way, chunk] = self.own[chunk].astype(bf16)
                self.copy(way, chunk, peer).start()

    def step(self, chunk, late):
        way, before, after, peer = self.flow(late)
        copy = self.copy(way, chunk, peer)

        @pl.when(jnp.logical_and(after, before))
        def _():
            copy.wait_recv()
            self.share[way, chunk] = (
                self.own[chunk] + self.land[way, chunk].astype(f32)
            ).astype(bf16)
            copy.start()

    def total(self, chunk):
        way, before, after, peer = self.flow(True)
        wait_recv_if(
            jnp.logical_and(before, jnp.logical_not(after)), self.copy(way, chunk, peer)
        )

        @pl.when(self.me > 0)
        def _():
            self.own[chunk] = self.own[chunk] + self.land[0, chunk].astype(f32)

        @pl.when(self.me < self.size - 1)
        def _():
            self.own[chunk] = self.own[chunk] + self.land[1, chunk].astype(f32)

    def drain(self):
        for late in (False, True):
            way, _, after, peer = self.flow(late)
            every = remote(
                self.share.at[way],
                self.land.at[way],
                self.send_sem.at[way],
                self.recv_sem.at[way, 0],
                batch=peer,
            )
            wait_send_if(after, every)


class PlaneScatter:
    def __init__(self, acc, land, send_sem, recv_sem, chip, core, bits, absolute=False):
        self.acc, self.land, self.absolute = acc, land, absolute
        self.send_sem, self.recv_sem = send_sem, recv_sem
        self.chip, self.core, self.bits = chip, core, bits
        self.slots, self.stages = [], []
        for half in range(2):
            order = [1 << bit for bit in range(bits)]
            order = order if half == 0 else order[::-1]
            used, slots, stages = 0, {}, []
            done = 0
            for stage, flip in enumerate(order):
                moved = [
                    block
                    for block in range((1 << bits) - 1, -1, -1)
                    if block & flip and not block & done
                ]
                for block in moved:
                    slots[(stage, block ^ flip)] = used
                    used += 1
                stages.append((flip, moved))
                done |= flip
            self.slots.append(slots)
            self.stages.append(stages)

    def place(self, block):
        return xor(self.chip, block, self.bits) if self.absolute else block

    def copy(self, half, stage, block):
        flip, _ = self.stages[half][stage]
        slot = self.slots[half][(stage, block ^ flip)]
        return remote(
            self.acc.at[self.place(block), half],
            self.land.at[slot, half],
            self.send_sem,
            self.recv_sem.at[slot, half],
            tensor=2 * xor(self.chip, flip, self.bits) + self.core,
        )

    def arrived(self, half, stages, block):
        return [
            self.land[self.slots[half][(stage, block)], half].astype(f32)
            for stage in range(stages)
        ]

    def send(self, stage, first=0, last=None):
        for half in range(2):
            for block in self.stages[half][stage][1][first:last]:
                place = self.place(block)
                if stage:
                    value = self.acc[place, half].astype(f32)
                    for term in self.arrived(half, stage, block):
                        value = value + term
                    self.acc[place, half] = value.astype(bf16)
                self.copy(half, stage, block).start()

    def receive(self, stage):
        for half in range(2):
            for block in self.stages[half][stage][1]:
                self.copy(half, stage, block).wait_recv()

    def final(self, half):
        value = self.acc[self.place(0), half].astype(f32)
        for term in self.arrived(half, self.bits, 0):
            value = value + term
        return value

    def drain(self):
        every = remote(
            self.land, self.land, self.send_sem, self.recv_sem.at[0, 0], tensor=self.core
        )
        every.wait_send()


def exchange_kernel(dims, *refs):
    (groups, tensors, mean_routed) = dims
    r = types.SimpleNamespace(**dict(zip(NAMES, refs, strict=True)))

    b, t = lax.axis_index("batch"), lax.axis_index("tensor")
    chips = tensors // 2
    bits = chips.bit_length() - 1
    chip, core = t // 2, lax.rem(t, 2)
    partner = t + 1 - 2 * core
    slots = r.route.shape[1]
    tokens, heads = r.attn.shape
    feats = r.out_weight.shape[1] // tensors
    width = r.student.shape[1]
    block = r.w_gate.shape[0]
    hidden_units = r.w_gate.shape[1]
    routed = mean_routed * groups
    tall = routed // 2
    short = routed // 4
    chunks = r.gu.shape[0] // 2
    cols = hidden_units // chunks
    portion = slots // chips
    others = range(1, chips)

    loads = {}

    def load(name, src, dst):
        copy = pltpu.make_async_copy(src, dst, r.load_sem.at[len(loads)])
        copy.start()
        loads[name] = copy

    def weight_block(index):
        place = pl.multiple_of(index * feats, feats)
        return r.out_weight.at[:, pl.ds(place, feats)]

    def owner(relative, side):
        return 2 * xor(chip, relative, bits) + (core if side else 1 - core)

    load("route", r.route, r.route_v)
    load("student", r.student, r.stud_v)
    load("attn", r.attn, r.attn_v.at[pl.ds(slots, tokens)])
    for side in range(2):
        for step in range(chips):
            place = side * chips + step
            index = owner(chips - 1 - step, side)
            load(("w", place), weight_block(index), r.weight_v.at[place])
    load("gain", r.gain, r.gain_v)
    load("w_gate", r.w_gate, r.wg)
    load("w_up", r.w_up, r.wu)
    load("residual", r.residual, r.resid_v)
    for side in range(2):
        for step in range(chips):
            index = 2 * step + (core if side else 1 - core)
            place = pl.multiple_of(index * width, width)
            load(
                ("p", side * chips + step),
                r.projector.at[:, pl.ds(place, width)],
                r.proj_v.at[side * chips + step],
            )
    load("w_down", r.w_down, r.wd)

    barrier = pltpu.get_barrier_semaphore()
    for step in others:
        pl.semaphore_signal(
            barrier,
            inc=1,
            device_id={"tensor": 2 * xor(chip, step, bits) + core},
            device_id_type=pl.DeviceIdType.MESH,
        )
    pl.semaphore_signal(
        barrier, inc=1, device_id={"tensor": partner}, device_id_type=pl.DeviceIdType.MESH
    )
    for step in range(1, groups):
        pl.semaphore_signal(
            barrier,
            inc=1,
            device_id={"batch": lax.rem(b + step, groups)},
            device_id_type=pl.DeviceIdType.MESH,
        )

    loads["route"].wait()
    route = r.route_v[...]
    row_id = lax.broadcasted_iota(jnp.int32, (slots, slots), 0)
    col_id = lax.broadcasted_iota(jnp.int32, (slots, slots), 1)
    route_col = jnp.sum(jnp.where(row_id == col_id, route, 0), axis=1, keepdims=True)
    token_id = lax.broadcasted_iota(jnp.int32, (slots, tokens), 1)
    pick = jnp.where(token_id == route_col, 1.0, 0.0).astype(bf16)
    count = jnp.sum(jnp.where(route >= 0, 1.0, 0.0), axis=1, keepdims=True)
    r.count_land[b] = jnp.broadcast_to(count, r.count_land.shape[1:])

    loads["student"].wait()
    r.x_land[0] = contract(pick, r.stud_v[...], 1, 0).astype(bf16)

    pl.semaphore_wait(barrier, chips - 1 + 1 + groups - 1)

    x_copies = [
        remote(
            r.x_land.at[0],
            r.x_land.at[step],
            r.out_sem.at[0],
            r.x_sem.at[step],
            tensor=2 * xor(chip, step, bits) + core,
        )
        for step in others
    ]
    for copy in x_copies[::-1]:
        copy.start()

    def count_copy(step):
        return remote(
            r.count_land.at[b],
            r.count_land.at[b],
            r.out_sem.at[1],
            r.count_sem.at[b],
            batch=lax.rem(b + step, groups),
        )

    for step in range(1, groups):
        count_copy(step).start()

    loads["attn"].wait()
    all_rows = slice(slots, slots + tokens)
    r.attn_v[0:slots] = contract(pick, r.attn_v[all_rows], 1, 0).astype(bf16)

    def pair_copy(send, land, sems, relative):
        out, sem = sems
        return remote(
            send.at[relative],
            land.at[relative],
            r.out_sem.at[out],
            sem.at[relative],
            tensor=partner,
        )

    piece = min(256, feats)

    def away(rows, send, land, sem, step):
        for place in range(0, feats, piece):
            span = slice(place, place + piece)
            value = jnp.dot(
                r.attn_v[rows], r.weight_v[step, :, span], preferred_element_type=f32
            )
            send[chips - 1 - step, :, span] = value.astype(bf16)
        pair_copy(send, land, sem, chips - 1 - step).start()

    def home(rows, send, land, sem, acc, step):
        relative = chips - 1 - step
        count = acc.shape[2]
        pair_copy(send, land, sem, relative).wait_recv()
        for place in range(0, feats, piece):
            span = slice(place, place + piece)
            value = jnp.dot(
                r.attn_v[rows], r.weight_v[chips + step, :, span], preferred_element_type=f32
            )
            value = (value + land[relative, :, span].astype(f32)).astype(bf16)
            for half in range(2):
                acc[relative, half, :, span] = value[half * count : (half + 1) * count]

    few = (slice(0, slots), r.q_send, r.q_land, (2, r.q_sem))
    many = (all_rows, r.t_send, r.t_land, (3, r.t_sem))
    routed_sum = PlaneScatter(
        r.r_acc, r.r_land, r.out_sem.at[5], r.r_sem, chip, core, bits
    )
    full_sum = PlaneScatter(
        r.f_acc, r.f_land, r.out_sem.at[6], r.f_sem, chip, core, bits
    )
    for step in range(chips):
        loads[("w", step)].wait()
        away(*few, step)
    for step in range(chips):
        loads[("w", chips + step)].wait()
        home(*few, r.r_acc, step)
    routed_sum.send(0)

    for copy in x_copies:
        copy.wait_recv()
    square = jnp.zeros((slots, 1), f32)
    for step in range(chips):
        value = r.x_land[step].astype(f32)
        square = square + jnp.sum(value * value, axis=1, keepdims=True)
    r.sq_send[...] = jnp.broadcast_to(square, r.sq_send.shape)
    sq_copy = remote(
        r.sq_send, r.sq_land, r.out_sem.at[15], r.sq_sem.at[0], tensor=partner
    )
    sq_copy.start()
    away(*many, 0)
    sq_copy.wait_recv()
    square = r.sq_send[:, 0:1] + r.sq_land[:, 0:1]
    loads["gain"].wait()
    scale = lax.rsqrt(square / (width * tensors) + epsilon)

    def z_copy(relative, peer):
        return remote(
            r.z_send.at[relative],
            r.z_land.at[b],
            r.out_sem.at[8],
            r.z_sem.at[b],
            batch=peer,
        )

    for relative in range(chips):
        peer = xor(chip, relative, bits)
        place = pl.multiple_of(peer * block + core * width, width)
        value = r.x_land[relative].astype(f32) * scale * r.gain_v[:, pl.ds(place, width)]
        value = value.astype(bf16)

        @pl.when(peer == b)
        def _():
            r.z_land[b] = value

        @pl.when(peer != b)
        def _():
            r.z_send[relative] = value
            z_copy(relative, peer).start()

    for step in range(1, chips):
        away(*many, step)
    home(*many, r.f_acc, 0)
    routed_sum.receive(0)
    routed_sum.send(1)
    for stage in range(2, bits):
        routed_sum.receive(stage - 1)
        routed_sum.send(stage)
    full_sum.send(0, 0, 1)
    for step in range(1, chips):
        home(*many, r.f_acc, step)

    for group in range(groups):
        for land, sem in ((r.count_land, r.count_sem), (r.z_land, r.z_sem)):
            wait_recv_if(
                group != b,
                remote(
                    land.at[group], land.at[group], r.out_sem.at[0], sem.at[group], batch=b
                ),
            )
    pack_row = lax.broadcasted_iota(jnp.int32, (routed, slots), 0).astype(f32)
    pack_col = lax.broadcasted_iota(jnp.int32, (routed, slots), 1).astype(f32)
    mine_row = lax.broadcasted_iota(jnp.int32, (routed, portion), 0).astype(f32)
    mine_col = lax.broadcasted_iota(jnp.int32, (routed, portion), 1) + chip * portion
    mine_col = mine_col.astype(f32)
    offset = jnp.zeros((1, 1), f32)
    packed = jnp.zeros((routed, width), f32)
    for group in range(groups):
        amount = r.count_land[group][0:1, 0:1]
        hit = jnp.logical_and(pack_col + offset == pack_row, pack_col < amount)
        packed = packed + contract(jnp.where(hit, 1.0, 0.0).astype(bf16), r.z_land[group], 1, 0)
        hit = jnp.logical_and(mine_col + offset == mine_row, mine_col < amount)
        r.select[group] = jnp.where(hit, 1.0, 0.0).astype(bf16)
        offset = offset + amount
    r.rows_v[core] = packed.astype(bf16)
    row_copy = remote(
        r.rows_v.at[core], r.rows_v.at[core], r.out_sem.at[16], r.row_sem.at[0], tensor=partner
    )
    row_copy.start()

    loads["w_gate"].wait()
    loads["w_up"].wait()

    out_gu = r.out_sem.at[pl.ds(10, 2)]
    gate_up = Chain(r.gu, r.gu_land, r.gu_share, out_gu, r.gu_sem, b, groups)

    def project(side, first):
        start = pl.multiple_of(side * width, width)
        rows = r.rows_v[side]
        for first_chunk in range(0, chunks, 2):
            span = slice(first_chunk * cols, (first_chunk + 2) * cols)
            for which, weight in enumerate((r.wg, r.wu)):
                value = jnp.dot(
                    rows, weight[pl.ds(start, width), span], preferred_element_type=f32
                )
                for turn, side_chunk in ((0, 0), (0, 1), (1, 0), (1, 1)):
                    item = turn * chunks + first_chunk + side_chunk
                    piece = value[
                        turn * tall : (turn + 1) * tall,
                        side_chunk * cols : (side_chunk + 1) * cols,
                    ]
                    r.gu[item, which] = piece if first else r.gu[item, which] + piece

    project(core, True)
    remote(
        r.rows_v.at[1 - core],
        r.rows_v.at[1 - core],
        r.out_sem.at[16],
        r.row_sem.at[0],
        tensor=partner,
    ).wait_recv()
    project(1 - core, False)
    gate_up.origin(0, chunks)
    for side in range(2):
        r.o_rows[:, side * width : (side + 1) * width] = r.rows_v[side]

    routed_sum.receive(bits - 1)
    loads["residual"].wait()
    routed_resid = contract(pick, r.resid_v[...], 1, 1)
    for half in range(2):
        first = half * (slots // 2)
        value = routed_sum.final(half) + routed_resid[first : first + slots // 2]
        r.p_keep[first : first + slots // 2] = value.astype(bf16)

    def target_copy(relative):
        return pair_copy(r.c_send, r.c_land, (4, r.c_sem), relative)

    for step in range(groups):
        loads[("p", step)].wait()
        value = jnp.dot(r.p_keep[...], r.proj_v[step], preferred_element_type=f32)
        r.c_send[step] = value.astype(bf16)
        target_copy(step).start()
    target_sum = PlaneScatter(
        r.p_acc, r.p_land, r.out_sem.at[7], r.p_sem, chip, core, bits, absolute=True
    )
    side_blocks = groups // 2

    def target_home():
        for step in range(groups):
            loads[("p", groups + step)].wait()
            value = jnp.dot(r.p_keep[...], r.proj_v[groups + step], preferred_element_type=f32)
            target_copy(step).wait_recv()
            value = (value + r.c_land[step].astype(f32)).astype(bf16)
            half, place = step // side_blocks, step % side_blocks * width
            for owner in range(chips):
                rows = value[owner * portion : (owner + 1) * portion]
                r.p_acc[owner, half, :, place : place + width] = rows
        target_sum.send(0)

    def target_relay():
        for stage in range(1, bits):
            target_sum.receive(stage - 1)
            target_sum.send(stage)

    def target_z(peer):
        return remote(
            r.p_send.at[peer],
            r.p_zland.at[b],
            r.out_sem.at[9],
            r.z2_sem.at[b],
            batch=peer,
        )

    def target_end():
        target_sum.receive(bits - 1)
        for half in range(2):
            value = target_sum.final(half).astype(bf16)
            for place in range(side_blocks):
                peer = half * side_blocks + place
                part = value[:, place * width : (place + 1) * width]

                @pl.when(peer == b)
                def _():
                    r.p_zland[b] = part

                @pl.when(peer != b)
                def _():
                    r.p_send[peer] = part
                    target_z(peer).start()

        full_sum.send(0, 1)

    def down(turn):
        rows = slice(turn * tall, (turn + 1) * tall)
        if turn == 0:
            loads["w_down"].wait()
        for chunk in range(chunks):
            item = turn * chunks + chunk
            gate_up.total(item)
            gate, up = r.gu[item, 0], r.gu[item, 1]
            value = (gate * jax.nn.sigmoid(gate) * up).astype(bf16)
            r.o_hidden[rows, chunk * cols : (chunk + 1) * cols] = value
            if chunk % 2:
                span = slice((chunk - 1) * cols, (chunk + 1) * cols)
                value = contract(r.o_hidden[rows, span], r.wd[:, span], 1, 1)
                r.part[turn] = value if chunk == 1 else r.part[turn] + value

        value = jnp.zeros((tall, width), f32)
        for group in range(groups):
            if turn == 0:
                wait_recv_if(
                    group != b,
                    remote(
                        r.p_zland.at[group],
                        r.p_zland.at[group],
                        r.out_sem.at[9],
                        r.z2_sem.at[group],
                        batch=b,
                    ),
                )
            value = value + contract(r.select[group, rows], r.p_zland[group], 1, 0)
        span = pl.ds(pl.multiple_of(core * width, width), width)
        r.part[turn, :, span] = r.part[turn, :, span] - value

    kept = pl.ds(pl.multiple_of(core * short, short), short)
    given = pl.ds(pl.multiple_of((1 - core) * short, short), short)
    half_cols = block // 2
    loss_scale = 1.0 / math.sqrt(routed)

    def misfit_copy(turn):
        return remote(
            r.m_send.at[turn],
            r.m_land.at[turn],
            r.out_sem.at[17 + turn],
            r.m_sem.at[turn],
            tensor=partner,
        )

    def double_copy(turn, stage, half):
        bit = stage if half == 0 else bits - 1 - stage
        return remote(
            r.v_share.at[turn, stage, half],
            r.v_land.at[turn, stage, half],
            r.out_sem.at[14],
            r.v_sem.at[turn, stage, half],
            tensor=2 * xor(chip, 1 << bit, bits) + core,
        )

    def grad_copy(turn, side):
        return remote(
            r.grad_v.at[turn, side],
            r.grad_v.at[turn, side],
            r.out_sem.at[19 + turn],
            r.g_sem.at[turn],
            tensor=partner,
        )

    def misfit_start(turn):
        r.m_send[turn] = r.part[turn, given].astype(bf16)
        misfit_copy(turn).start()

    def double_start(turn, stage):
        if stage == 0:
            misfit_copy(turn).wait_recv()
            total = r.part[turn, kept] + r.m_land[turn].astype(f32)
            values = [total[:, :half_cols], total[:, half_cols:]]
        else:
            values = doubled(turn, stage - 1)
        for half in range(2):
            r.v_share[turn, stage, half] = values[half].astype(bf16)
            double_copy(turn, stage, half).start()

    def doubled(turn, stage):
        values = []
        for half in range(2):
            double_copy(turn, stage, half).wait_recv()
            values.append(
                r.v_share[turn, stage, half].astype(f32)
                + r.v_land[turn, stage, half].astype(f32)
            )
        return values

    def grad_start(turn):
        values = doubled(turn, bits - 1)
        for half in range(2):
            span = slice(half * half_cols, (half + 1) * half_cols)
            r.grad_v[turn, core, :, span] = (values[half] * loss_scale).astype(bf16)
        grad_copy(turn, core).start()

    out_gh = r.out_sem.at[pl.ds(12, 2)]
    grad_hidden = Chain(r.gh, r.gh_land, r.gh_share, out_gh, r.gh_sem, b, groups)

    def back(turn):
        grad_copy(turn, 1 - core).wait_recv()
        for side in range(2):
            first = turn * tall + side * short
            r.o_grad[first : first + short] = r.grad_v[turn, side]
        rows = slice(turn * tall, (turn + 1) * tall)
        for chunk in range(0, chunks, 2):
            span = slice(chunk * cols, (chunk + 2) * cols)
            value = jnp.dot(r.o_grad[rows], r.wd[:, span], preferred_element_type=f32)
            for side in range(2):
                item = turn * chunks + chunk + side
                r.gh[item] = value[:, side * cols : (side + 1) * cols]
        grad_hidden.origin(turn * chunks, (turn + 1) * chunks)

    def last(turn):
        rows = slice(turn * tall, (turn + 1) * tall)
        for chunk in range(chunks):
            item = turn * chunks + chunk
            grad_hidden.total(item)
            span = slice(chunk * cols, (chunk + 1) * cols)
            gate, up, grad = r.gu[item, 0], r.gu[item, 1], r.gh[item]
            sigma = jax.nn.sigmoid(gate)
            r.o_gate[rows, span] = (
                grad * up * sigma * (1.0 + gate * (1.0 - sigma))
            ).astype(bf16)
            r.o_up[rows, span] = (grad * gate * sigma).astype(bf16)

    def steps(chain, *items):
        for late, item in items:
            chain.step(item, bool(late))

    def order_of(first, final, skew):
        order = []
        for step in range(first, final + skew):
            if step < final:
                order.append((0, step))
            if step - skew >= first:
                order.append((1, step - skew))
        return order

    items = 2 * chunks
    order = order_of(0, items, min(5, chunks))
    late = [order.index((1, item)) + 1 for item in range(items)]

    target_home()
    gate_up.origin(chunks, items)
    steps(gate_up, *order[: late[0] - 1])
    target_relay()
    steps(gate_up, *order[late[0] - 1 : late[chunks - 3]])
    target_end()
    begin = min(items - 2, chunks + 1)
    steps(gate_up, *order[late[chunks - 3] : late[begin]])
    down(0)
    misfit_start(0)
    for stage in range(bits):
        end = min(items - 1, begin + 2)
        steps(gate_up, *order[late[begin] : late[end]])
        double_start(0, stage)
        begin = end
    steps(gate_up, *order[late[begin] :])
    down(1)
    misfit_start(1)
    grad_start(0)
    double_start(1, 0)
    back(0)

    order = order_of(0, chunks, chunks)
    late = [order.index((1, item)) + 1 for item in range(chunks)]
    steps(grad_hidden, *order[:2])
    for stage in range(1, bits):
        double_start(1, stage)
    steps(grad_hidden, *order[2 : late[0] - 1])
    grad_start(1)
    for stage in range(1, bits):
        full_sum.receive(stage - 1)
        full_sum.send(stage)
    steps(grad_hidden, *order[late[0] - 1 : late[3]])
    back(1)
    steps(grad_hidden, *order[late[3] :])
    last(0)
    steps(grad_hidden, *order_of(chunks, items, chunks))
    last(1)

    full_sum.receive(bits - 1)
    for half in range(2):
        span = slice(half * (tokens // 2), (half + 1) * (tokens // 2))
        value = full_sum.final(half).T + r.resid_v[:, span].astype(f32)
        r.o_teacher[:, span] = value.astype(bf16)

    some = pl.ds(1, chips - 1)
    sent = (
        (0, r.x_land.at[some]),
        (1, r.count_land.at[some]),
        (2, r.q_send),
        (3, r.t_send),
        (4, r.c_send),
        (8, r.z_send.at[some]),
        (9, r.p_send.at[some]),
        (14, r.v_share),
    )
    for out, array in sent:
        remote(array, array, r.out_sem.at[out], r.sq_sem.at[0], tensor=partner).wait_send()
    sq_copy.wait_send()
    row_copy.wait_send()
    for turn in range(2):
        misfit_copy(turn).wait_send()
        grad_copy(turn, core).wait_send()
    routed_sum.drain()
    target_sum.drain()
    full_sum.drain()
    gate_up.drain()
    grad_hidden.drain()


def grads_kernel(
    rows, gate, up, grad, hidden, teacher, o_gate, o_up, o_down, o_teacher, hold, sem, end_sem
):
    count, parts, tall, _ = hold.shape
    copies = [pltpu.make_async_copy(teacher, o_teacher, end_sem.at[0])]
    copies[0].start()
    terms = ((grad, hidden, o_down), (rows, gate, o_gate), (rows, up, o_up))
    for which, (left, right, out) in enumerate(terms):
        for part in range(parts):
            span = pl.ds(part * tall, tall)
            hold[which, part] = contract(left[:, span], right[...], 0, 0)
            copy = pltpu.make_async_copy(hold.at[which, part], out.at[span], sem.at[which, part])
            copy.start()
            copies.append(copy)
    for copy in copies:
        copy.wait()


def on_device(
    attn_values,
    out_weight,
    residual_t,
    projector,
    student_input,
    norm_gain,
    w_gate,
    w_up,
    w_down,
    route_index,
):
    groups, tensors = lax.axis_size("batch"), lax.axis_size("tensor")
    chips = tensors // 2
    bits = chips.bit_length() - 1
    if chips != groups or 1 << bits != chips:
        raise ValueError("mesh")
    mean_routed = student_input.shape[0] // 8
    routed = mean_routed * groups
    tokens, heads = attn_values.shape
    feats = out_weight.shape[1] // tensors
    model = projector.shape[1]
    width = student_input.shape[1]
    block, units = w_gate.shape
    slots = route_index.shape[1]
    cols = min(128, units)
    chunks = units // cols
    dma = pltpu.SemaphoreType.DMA
    moved = chips - 1
    scratch = [
        pltpu.VMEM((slots + tokens, heads), bf16),
        pltpu.VMEM((tensors, heads, feats), bf16),
        pltpu.VMEM(residual_t.shape, bf16),
        pltpu.VMEM((tensors, feats, width), bf16),
        pltpu.VMEM(student_input.shape, bf16),
        pltpu.VMEM(w_gate.shape, bf16),
        pltpu.VMEM(w_up.shape, bf16),
        pltpu.VMEM(w_down.shape, bf16),
        pltpu.VMEM(route_index.shape, route_index.dtype),
        pltpu.VMEM((1, model), f32),
        dma((8 + 2 * tensors,)),
        dma((21,)),
        pltpu.VMEM((chips, slots, feats), bf16),
        pltpu.VMEM((chips, slots, feats), bf16),
        dma((chips,)),
        pltpu.VMEM((chips, tokens, feats), bf16),
        pltpu.VMEM((chips, tokens, feats), bf16),
        pltpu.VMEM((chips, 2, slots // 2, feats), bf16),
        pltpu.VMEM((moved, 2, slots // 2, feats), bf16),
        pltpu.VMEM((chips, 2, tokens // 2, feats), bf16),
        pltpu.VMEM((moved, 2, tokens // 2, feats), bf16),
        dma((chips,)),
        dma((moved, 2)),
        dma((moved, 2)),
        pltpu.VMEM((chips, slots, width), bf16),
        pltpu.VMEM((chips, slots, width), bf16),
        pltpu.VMEM((chips, 2, slots // chips, model // 4), bf16),
        pltpu.VMEM((moved, 2, slots // chips, model // 4), bf16),
        pltpu.VMEM((slots, feats), bf16),
        pltpu.VMEM((groups, slots // chips, width), bf16),
        pltpu.VMEM((groups, slots // chips, width), bf16),
        dma((chips,)),
        dma((moved, 2)),
        dma((groups,)),
        pltpu.VMEM((chips, slots, width), bf16),
        pltpu.VMEM((slots, 128), f32),
        pltpu.VMEM((slots, 128), f32),
        pltpu.VMEM((groups, 8, 128), f32),
        dma((chips,)),
        dma((2,)),
        dma((groups,)),
        pltpu.VMEM((chips, slots, width), bf16),
        pltpu.VMEM((groups, slots, width), bf16),
        dma((groups,)),
        pltpu.VMEM((groups, routed, slots // chips), bf16),
        pltpu.VMEM((2, routed, width), bf16),
        dma((2,)),
        pltpu.VMEM((2 * chunks, 2, routed // 2, cols), f32),
        pltpu.VMEM((2, 2 * chunks, 2, routed // 2, cols), bf16),
        pltpu.VMEM((2, 2 * chunks, 2, routed // 2, cols), bf16),
        dma((2, 2 * chunks)),
        pltpu.VMEM((2 * chunks, routed // 2, cols), f32),
        pltpu.VMEM((2, 2 * chunks, routed // 2, cols), bf16),
        pltpu.VMEM((2, 2 * chunks, routed // 2, cols), bf16),
        dma((2, 2 * chunks)),
        pltpu.VMEM((2, routed // 2, block), f32),
        pltpu.VMEM((2, routed // 4, block), bf16),
        pltpu.VMEM((2, routed // 4, block), bf16),
        pltpu.VMEM((2, bits, 2, routed // 4, block // 2), bf16),
        pltpu.VMEM((2, bits, 2, routed // 4, block // 2), bf16),
        dma((2,)),
        dma((2, bits, 2)),
        pltpu.VMEM((2, 2, routed // 4, block), bf16),
        dma((2,)),
    ]
    rows, gate, up, grad, hidden, teacher = pl.pallas_call(
        functools.partial(exchange_kernel, (groups, tensors, mean_routed)),
        name="exchange",
        out_shape=(
            jax.ShapeDtypeStruct((routed, block), bf16),
            jax.ShapeDtypeStruct((routed, units), bf16),
            jax.ShapeDtypeStruct((routed, units), bf16),
            jax.ShapeDtypeStruct((routed, block), bf16),
            jax.ShapeDtypeStruct((routed, units), bf16),
            jax.ShapeDtypeStruct(residual_t.shape, bf16),
        ),
        in_specs=[HBM] * 10,
        out_specs=[VMEM] * 6,
        scratch_shapes=scratch,
        compiler_params=pltpu.CompilerParams(
            collective_id=1, has_side_effects=True, vmem_limit_bytes=VMEM_BYTES
        ),
    )(
        attn_values,
        out_weight,
        residual_t,
        projector,
        student_input,
        norm_gain.reshape(1, -1),
        w_gate,
        w_up,
        w_down,
        route_index,
    )
    parts = 4
    grads = jax.ShapeDtypeStruct((block, units), f32)
    grad_gate, grad_up, grad_down, teacher_hidden = pl.pallas_call(
        grads_kernel,
        name="grads",
        out_shape=(grads, grads, grads, jax.ShapeDtypeStruct(residual_t.shape, bf16)),
        in_specs=[VMEM] * 6,
        out_specs=[HBM] * 4,
        scratch_shapes=[
            pltpu.VMEM((3, parts, block // parts, units), f32),
            dma((3, parts)),
            dma((1,)),
        ],
        compiler_params=pltpu.CompilerParams(vmem_limit_bytes=20_000_000),
    )(rows, gate, up, grad, hidden, teacher)
    return (teacher_hidden, grad_gate, grad_up, grad_down)


def solution(mesh):
    in_specs = (
        P("batch", "tensor"),
        P("tensor", None),
        P("tensor", "batch"),
        P("tensor", None),
        P("batch", "tensor"),
        P(),
        P("batch", "tensor"),
        P("batch", "tensor"),
        P("batch", "tensor"),
        P("batch", None),
    )
    out_specs = (
        P("tensor", "batch"),
        P("batch", "tensor"),
        P("batch", "tensor"),
        P("batch", "tensor"),
    )
    return jax.shard_map(
        on_device, mesh=mesh, in_specs=in_specs, out_specs=out_specs, check_vma=False
    )
```

```python
import functools
import math
import types

import jax
import jax.numpy as jnp
from jax import lax
from jax.experimental import pallas as pl
from jax.experimental.pallas import tpu as pltpu
from jax.sharding import PartitionSpec as P

epsilon = 1e-05
f32 = jnp.float32
bf16 = jnp.bfloat16
VMEM = pl.BlockSpec(memory_space=pltpu.VMEM)
HBM = pl.BlockSpec(memory_space=pltpu.HBM)
VMEM_BYTES = 54_000_000

NAMES = (
    "attn", "out_weight", "residual", "projector", "student", "gain", "w_gate", "w_up",
    "w_down", "route", "o_rows", "o_gate", "o_up", "o_grad", "o_hidden", "o_teacher",
    "attn_v", "weight_v", "resid_v", "proj_v", "stud_v", "wg", "wu", "wd", "route_v", "gain_v",
    "load_sem", "out_sem",
    "q_send", "q_land", "q_sem", "t_send", "t_land", "r_acc", "r_land", "f_acc", "f_land", "t_sem", "r_sem", "f_sem",
    "c_send", "c_land", "p_acc", "p_land", "p_keep", "p_send", "p_zland", "c_sem", "p_sem", "z2_sem",
    "x_land", "sq_send", "sq_land", "count_land", "x_sem", "sq_sem", "count_sem", "z_send",
    "z_land", "z_sem", "select", "rows_v", "row_sem", "gu", "gu_land", "gu_share", "gu_sem", "gh",
    "gh_land", "gh_share", "gh_sem", "part", "m_send", "m_land", "v_share", "v_land", "m_sem",
    "v_sem", "grad_v", "g_sem",
)


def contract(left, right, left_dim, right_dim):
    return lax.dot_general(
        left, right, (((left_dim,), (right_dim,)), ((), ())), preferred_element_type=f32
    )


def remote(src, dst, send_sem, recv_sem, **where):
    return pltpu.make_async_remote_copy(
        src_ref=src,
        dst_ref=dst,
        send_sem=send_sem,
        recv_sem=recv_sem,
        device_id=where,
        device_id_type=pl.DeviceIdType.MESH,
    )


def start_if(cond, copy):
    @pl.when(cond)
    def _():
        copy.start()


def wait_send_if(cond, copy):
    @pl.when(cond)
    def _():
        copy.wait_send()


def wait_recv_if(cond, copy):
    @pl.when(cond)
    def _():
        copy.wait_recv()


def xor(left, right, bits):
    total = 0
    for bit in range(bits):
        step = 1 << bit
        total = total + step * lax.rem(left // step + right // step, 2)
    return total


class Chain:
    def __init__(self, own, land, share, send_sem, recv_sem, me, size):
        self.own, self.land, self.share = own, land, share
        self.send_sem, self.recv_sem = send_sem, recv_sem
        self.me, self.size, self.chunks = me, size, own.shape[0]
        self.early = jnp.where(2 * me < size, 0, 1)

    def flow(self, late):
        way = 1 - self.early if late else self.early
        before = jnp.where(way == 0, self.me, self.size - 1 - self.me) > 0
        after = jnp.where(way == 0, self.size - 1 - self.me, self.me) > 0
        peer = jnp.where(way == 0, self.me + 1, self.me - 1)
        return way, before, after, peer

    def copy(self, way, chunk, peer):
        return remote(
            self.share.at[way, chunk],
            self.land.at[way, chunk],
            self.send_sem.at[way],
            self.recv_sem.at[way, chunk],
            batch=peer,
        )

    def origin(self, first, last):
        way, before, after, peer = self.flow(False)

        @pl.when(jnp.logical_not(before))
        def _():
            for chunk in range(first, last):
                self.share[way, chunk] = self.own[chunk].astype(bf16)
                self.copy(way, chunk, peer).start()

    def step(self, chunk, late):
        way, before, after, peer = self.flow(late)
        copy = self.copy(way, chunk, peer)

        @pl.when(jnp.logical_and(after, before))
        def _():
            copy.wait_recv()
            self.share[way, chunk] = (
                self.own[chunk] + self.land[way, chunk].astype(f32)
            ).astype(bf16)
            copy.start()

    def total(self, chunk):
        way, before, after, peer = self.flow(True)
        wait_recv_if(
            jnp.logical_and(before, jnp.logical_not(after)), self.copy(way, chunk, peer)
        )

        @pl.when(self.me > 0)
        def _():
            self.own[chunk] = self.own[chunk] + self.land[0, chunk].astype(f32)

        @pl.when(self.me < self.size - 1)
        def _():
            self.own[chunk] = self.own[chunk] + self.land[1, chunk].astype(f32)

    def drain(self):
        for late in (False, True):
            way, _, after, peer = self.flow(late)
            every = remote(
                self.share.at[way],
                self.land.at[way],
                self.send_sem.at[way],
                self.recv_sem.at[way, 0],
                batch=peer,
            )
            wait_send_if(after, every)


class PlaneScatter:
    def __init__(self, acc, land, send_sem, recv_sem, chip, core, bits, absolute=False):
        self.acc, self.land, self.absolute = acc, land, absolute
        self.send_sem, self.recv_sem = send_sem, recv_sem
        self.chip, self.core, self.bits = chip, core, bits
        self.slots, self.stages = [], []
        for half in range(2):
            order = [1 << bit for bit in range(bits)]
            order = order if half == 0 else order[::-1]
            used, slots, stages = 0, {}, []
            done = 0
            for stage, flip in enumerate(order):
                moved = [
                    block
                    for block in range((1 << bits) - 1, -1, -1)
                    if block & flip and not block & done
                ]
                for block in moved:
                    slots[(stage, block ^ flip)] = used
                    used += 1
                stages.append((flip, moved))
                done |= flip
            self.slots.append(slots)
            self.stages.append(stages)

    def place(self, block):
        return xor(self.chip, block, self.bits) if self.absolute else block

    def copy(self, half, stage, block):
        flip, _ = self.stages[half][stage]
        slot = self.slots[half][(stage, block ^ flip)]
        return remote(
            self.acc.at[self.place(block), half],
            self.land.at[slot, half],
            self.send_sem,
            self.recv_sem.at[slot, half],
            tensor=2 * xor(self.chip, flip, self.bits) + self.core,
        )

    def arrived(self, half, stages, block):
        return [
            self.land[self.slots[half][(stage, block)], half].astype(f32)
            for stage in range(stages)
        ]

    def send(self, stage, first=0, last=None):
        for half in range(2):
            for block in self.stages[half][stage][1][first:last]:
                place = self.place(block)
                if stage:
                    value = self.acc[place, half].astype(f32)
                    for term in self.arrived(half, stage, block):
                        value = value + term
                    self.acc[place, half] = value.astype(bf16)
                self.copy(half, stage, block).start()

    def receive(self, stage):
        for half in range(2):
            for block in self.stages[half][stage][1]:
                self.copy(half, stage, block).wait_recv()

    def final(self, half):
        value = self.acc[self.place(0), half].astype(f32)
        for term in self.arrived(half, self.bits, 0):
            value = value + term
        return value

    def drain(self):
        every = remote(
            self.land, self.land, self.send_sem, self.recv_sem.at[0, 0], tensor=self.core
        )
        every.wait_send()


def exchange_kernel(dims, *refs):
    (groups, tensors, mean_routed) = dims
    r = types.SimpleNamespace(**dict(zip(NAMES, refs, strict=True)))

    b, t = lax.axis_index("batch"), lax.axis_index("tensor")
    chips = tensors // 2
    bits = chips.bit_length() - 1
    chip, core = t // 2, lax.rem(t, 2)
    partner = t + 1 - 2 * core
    slots = r.route.shape[1]
    tokens, heads = r.attn.shape
    feats = r.out_weight.shape[1] // tensors
    width = r.student.shape[1]
    block = r.w_gate.shape[0]
    hidden_units = r.w_gate.shape[1]
    routed = mean_routed * groups
    tall = routed // 2
    short = routed // 4
    chunks = r.gu.shape[0] // 2
    cols = hidden_units // chunks
    portion = slots // chips
    others = range(1, chips)

    loads = {}

    def load(name, src, dst):
        copy = pltpu.make_async_copy(src, dst, r.load_sem.at[len(loads)])
        copy.start()
        loads[name] = copy

    def weight_block(index):
        place = pl.multiple_of(index * feats, feats)
        return r.out_weight.at[:, pl.ds(place, feats)]

    def owner(relative, side):
        return 2 * xor(chip, relative, bits) + (core if side else 1 - core)

    load("route", r.route, r.route_v)
    load("student", r.student, r.stud_v)
    load("attn", r.attn, r.attn_v.at[pl.ds(slots, tokens)])
    for side in range(2):
        for step in range(chips):
            place = side * chips + step
            index = owner(chips - 1 - step, side)
            load(("w", place), weight_block(index), r.weight_v.at[place])
    load("gain", r.gain, r.gain_v)
    load("w_gate", r.w_gate, r.wg)
    load("w_up", r.w_up, r.wu)
    load("residual", r.residual, r.resid_v)
    for side in range(2):
        for step in range(chips):
            index = 2 * step + (core if side else 1 - core)
            place = pl.multiple_of(index * width, width)
            load(
                ("p", side * chips + step),
                r.projector.at[:, pl.ds(place, width)],
                r.proj_v.at[side * chips + step],
            )
    load("w_down", r.w_down, r.wd)

    barrier = pltpu.get_barrier_semaphore()
    for step in others:
        pl.semaphore_signal(
            barrier,
            inc=1,
            device_id={"tensor": 2 * xor(chip, step, bits) + core},
            device_id_type=pl.DeviceIdType.MESH,
        )
    pl.semaphore_signal(
        barrier, inc=1, device_id={"tensor": partner}, device_id_type=pl.DeviceIdType.MESH
    )
    for step in range(1, groups):
        pl.semaphore_signal(
            barrier,
            inc=1,
            device_id={"batch": lax.rem(b + step, groups)},
            device_id_type=pl.DeviceIdType.MESH,
        )

    loads["route"].wait()
    route = r.route_v[...]
    row_id = lax.broadcasted_iota(jnp.int32, (slots, slots), 0)
    col_id = lax.broadcasted_iota(jnp.int32, (slots, slots), 1)
    route_col = jnp.sum(jnp.where(row_id == col_id, route, 0), axis=1, keepdims=True)
    token_id = lax.broadcasted_iota(jnp.int32, (slots, tokens), 1)
    pick = jnp.where(token_id == route_col, 1.0, 0.0).astype(bf16)
    count = jnp.sum(jnp.where(route >= 0, 1.0, 0.0), axis=1, keepdims=True)
    r.count_land[b] = jnp.broadcast_to(count, r.count_land.shape[1:])

    loads["student"].wait()
    r.x_land[0] = contract(pick, r.stud_v[...], 1, 0).astype(bf16)

    pl.semaphore_wait(barrier, chips - 1 + 1 + groups - 1)

    x_copies = [
        remote(
            r.x_land.at[0],
            r.x_land.at[step],
            r.out_sem.at[0],
            r.x_sem.at[step],
            tensor=2 * xor(chip, step, bits) + core,
        )
        for step in others
    ]
    for copy in x_copies[::-1]:
        copy.start()

    def count_copy(step):
        return remote(
            r.count_land.at[b],
            r.count_land.at[b],
            r.out_sem.at[1],
            r.count_sem.at[b],
            batch=lax.rem(b + step, groups),
        )

    for step in range(1, groups):
        count_copy(step).start()

    loads["attn"].wait()
    all_rows = slice(slots, slots + tokens)
    r.attn_v[0:slots] = contract(pick, r.attn_v[all_rows], 1, 0).astype(bf16)

    def pair_copy(send, land, sems, relative):
        out, sem = sems
        return remote(
            send.at[relative],
            land.at[relative],
            r.out_sem.at[out],
            sem.at[relative],
            tensor=partner,
        )

    piece = min(256, feats)

    def away(rows, send, land, sem, step):
        for place in range(0, feats, piece):
            span = slice(place, place + piece)
            value = jnp.dot(
                r.attn_v[rows], r.weight_v[step, :, span], preferred_element_type=f32
            )
            send[chips - 1 - step, :, span] = value.astype(bf16)
        pair_copy(send, land, sem, chips - 1 - step).start()

    def home(rows, send, land, sem, acc, step):
        relative = chips - 1 - step
        count = acc.shape[2]
        pair_copy(send, land, sem, relative).wait_recv()
        for place in range(0, feats, piece):
            span = slice(place, place + piece)
            value = jnp.dot(
                r.attn_v[rows], r.weight_v[chips + step, :, span], preferred_element_type=f32
            )
            value = (value + land[relative, :, span].astype(f32)).astype(bf16)
            for half in range(2):
                acc[relative, half, :, span] = value[half * count : (half + 1) * count]

    few = (slice(0, slots), r.q_send, r.q_land, (2, r.q_sem))
    many = (all_rows, r.t_send, r.t_land, (3, r.t_sem))
    routed_sum = PlaneScatter(
        r.r_acc, r.r_land, r.out_sem.at[5], r.r_sem, chip, core, bits
    )
    full_sum = PlaneScatter(
        r.f_acc, r.f_land, r.out_sem.at[6], r.f_sem, chip, core, bits
    )
    for step in range(chips):
        loads[("w", step)].wait()
        away(*few, step)
    for step in range(chips):
        loads[("w", chips + step)].wait()
        home(*few, r.r_acc, step)
    routed_sum.send(0)

    for copy in x_copies:
        copy.wait_recv()
    square = jnp.zeros((slots, 1), f32)
    for step in range(chips):
        value = r.x_land[step].astype(f32)
        square = square + jnp.sum(value * value, axis=1, keepdims=True)
    r.sq_send[...] = jnp.broadcast_to(square, r.sq_send.shape)
    sq_copy = remote(
        r.sq_send, r.sq_land, r.out_sem.at[15], r.sq_sem.at[0], tensor=partner
    )
    sq_copy.start()
    away(*many, 0)
    sq_copy.wait_recv()
    square = r.sq_send[:, 0:1] + r.sq_land[:, 0:1]
    loads["gain"].wait()
    scale = lax.rsqrt(square / (width * tensors) + epsilon)

    def z_copy(relative, peer):
        return remote(
            r.z_send.at[relative],
            r.z_land.at[b],
            r.out_sem.at[8],
            r.z_sem.at[b],
            batch=peer,
        )

    for relative in range(chips):
        peer = xor(chip, relative, bits)
        place = pl.multiple_of(peer * block + core * width, width)
        value = r.x_land[relative].astype(f32) * scale * r.gain_v[:, pl.ds(place, width)]
        value = value.astype(bf16)

        @pl.when(peer == b)
        def _():
            r.z_land[b] = value

        @pl.when(peer != b)
        def _():
            r.z_send[relative] = value
            z_copy(relative, peer).start()

    for step in range(1, chips):
        away(*many, step)
    home(*many, r.f_acc, 0)
    routed_sum.receive(0)
    routed_sum.send(1)
    for stage in range(2, bits):
        routed_sum.receive(stage - 1)
        routed_sum.send(stage)
    full_sum.send(0, 0, 1)
    for step in range(1, chips):
        home(*many, r.f_acc, step)

    for group in range(groups):
        for land, sem in ((r.count_land, r.count_sem), (r.z_land, r.z_sem)):
            wait_recv_if(
                group != b,
                remote(
                    land.at[group], land.at[group], r.out_sem.at[0], sem.at[group], batch=b
                ),
            )
    pack_row = lax.broadcasted_iota(jnp.int32, (routed, slots), 0).astype(f32)
    pack_col = lax.broadcasted_iota(jnp.int32, (routed, slots), 1).astype(f32)
    mine_row = lax.broadcasted_iota(jnp.int32, (routed, portion), 0).astype(f32)
    mine_col = lax.broadcasted_iota(jnp.int32, (routed, portion), 1) + chip * portion
    mine_col = mine_col.astype(f32)
    offset = jnp.zeros((1, 1), f32)
    packed = jnp.zeros((routed, width), f32)
    for group in range(groups):
        amount = r.count_land[group][0:1, 0:1]
        hit = jnp.logical_and(pack_col + offset == pack_row, pack_col < amount)
        packed = packed + contract(jnp.where(hit, 1.0, 0.0).astype(bf16), r.z_land[group], 1, 0)
        hit = jnp.logical_and(mine_col + offset == mine_row, mine_col < amount)
        r.select[group] = jnp.where(hit, 1.0, 0.0).astype(bf16)
        offset = offset + amount
    r.rows_v[core] = packed.astype(bf16)
    row_copy = remote(
        r.rows_v.at[core], r.rows_v.at[core], r.out_sem.at[16], r.row_sem.at[0], tensor=partner
    )
    row_copy.start()

    loads["w_gate"].wait()
    loads["w_up"].wait()

    out_gu = r.out_sem.at[pl.ds(10, 2)]
    gate_up = Chain(r.gu, r.gu_land, r.gu_share, out_gu, r.gu_sem, b, groups)

    def project(side, first):
        start = pl.multiple_of(side * width, width)
        rows = r.rows_v[side]
        for first_chunk in range(0, chunks, 2):
            span = slice(first_chunk * cols, (first_chunk + 2) * cols)
            for which, weight in enumerate((r.wg, r.wu)):
                value = jnp.dot(
                    rows, weight[pl.ds(start, width), span], preferred_element_type=f32
                )
                for turn, side_chunk in ((0, 0), (0, 1), (1, 0), (1, 1)):
                    item = turn * chunks + first_chunk + side_chunk
                    piece = value[
                        turn * tall : (turn + 1) * tall,
                        side_chunk * cols : (side_chunk + 1) * cols,
                    ]
                    r.gu[item, which] = piece if first else r.gu[item, which] + piece

    project(core, True)
    remote(
        r.rows_v.at[1 - core],
        r.rows_v.at[1 - core],
        r.out_sem.at[16],
        r.row_sem.at[0],
        tensor=partner,
    ).wait_recv()
    project(1 - core, False)
    gate_up.origin(0, chunks)
    for side in range(2):
        r.o_rows[:, side * width : (side + 1) * width] = r.rows_v[side]

    routed_sum.receive(bits - 1)
    loads["residual"].wait()
    routed_resid = contract(pick, r.resid_v[...], 1, 1)
    for half in range(2):
        first = half * (slots // 2)
        value = routed_sum.final(half) + routed_resid[first : first + slots // 2]
        r.p_keep[first : first + slots // 2] = value.astype(bf16)

    def target_copy(relative):
        return pair_copy(r.c_send, r.c_land, (4, r.c_sem), relative)

    for step in range(groups):
        loads[("p", step)].wait()
        value = jnp.dot(r.p_keep[...], r.proj_v[step], preferred_element_type=f32)
        r.c_send[step] = value.astype(bf16)
        target_copy(step).start()
    target_sum = PlaneScatter(
        r.p_acc, r.p_land, r.out_sem.at[7], r.p_sem, chip, core, bits, absolute=True
    )
    side_blocks = groups // 2

    def target_home():
        for step in range(groups):
            loads[("p", groups + step)].wait()
            value = jnp.dot(r.p_keep[...], r.proj_v[groups + step], preferred_element_type=f32)
            target_copy(step).wait_recv()
            value = (value + r.c_land[step].astype(f32)).astype(bf16)
            half, place = step // side_blocks, step % side_blocks * width
            for owner in range(chips):
                rows = value[owner * portion : (owner + 1) * portion]
                r.p_acc[owner, half, :, place : place + width] = rows
        target_sum.send(0)

    def target_relay():
        for stage in range(1, bits):
            target_sum.receive(stage - 1)
            target_sum.send(stage)

    def target_z(peer):
        return remote(
            r.p_send.at[peer],
            r.p_zland.at[b],
            r.out_sem.at[9],
            r.z2_sem.at[b],
            batch=peer,
        )

    def target_end():
        target_sum.receive(bits - 1)
        for half in range(2):
            value = target_sum.final(half).astype(bf16)
            for place in range(side_blocks):
                peer = half * side_blocks + place
                part = value[:, place * width : (place + 1) * width]

                @pl.when(peer == b)
                def _():
                    r.p_zland[b] = part

                @pl.when(peer != b)
                def _():
                    r.p_send[peer] = part
                    target_z(peer).start()

        full_sum.send(0, 1)

    def down(turn):
        rows = slice(turn * tall, (turn + 1) * tall)
        if turn == 0:
            loads["w_down"].wait()
        for chunk in range(chunks):
            item = turn * chunks + chunk
            gate_up.total(item)
            gate, up = r.gu[item, 0], r.gu[item, 1]
            value = (gate * jax.nn.sigmoid(gate) * up).astype(bf16)
            r.o_hidden[rows, chunk * cols : (chunk + 1) * cols] = value
            if chunk % 2:
                span = slice((chunk - 1) * cols, (chunk + 1) * cols)
                value = contract(r.o_hidden[rows, span], r.wd[:, span], 1, 1)
                r.part[turn] = value if chunk == 1 else r.part[turn] + value

        value = jnp.zeros((tall, width), f32)
        for group in range(groups):
            if turn == 0:
                wait_recv_if(
                    group != b,
                    remote(
                        r.p_zland.at[group],
                        r.p_zland.at[group],
                        r.out_sem.at[9],
                        r.z2_sem.at[group],
                        batch=b,
                    ),
                )
            value = value + contract(r.select[group, rows], r.p_zland[group], 1, 0)
        span = pl.ds(pl.multiple_of(core * width, width), width)
        r.part[turn, :, span] = r.part[turn, :, span] - value

    kept = pl.ds(pl.multiple_of(core * short, short), short)
    given = pl.ds(pl.multiple_of((1 - core) * short, short), short)
    half_cols = block // 2
    loss_scale = 1.0 / math.sqrt(routed)

    def misfit_copy(turn):
        return remote(
            r.m_send.at[turn],
            r.m_land.at[turn],
            r.out_sem.at[17 + turn],
            r.m_sem.at[turn],
            tensor=partner,
        )

    def double_copy(turn, stage, half):
        bit = stage if half == 0 else bits - 1 - stage
        return remote(
            r.v_share.at[turn, stage, half],
            r.v_land.at[turn, stage, half],
            r.out_sem.at[14],
            r.v_sem.at[turn, stage, half],
            tensor=2 * xor(chip, 1 << bit, bits) + core,
        )

    def grad_copy(turn, side):
        return remote(
            r.grad_v.at[turn, side],
            r.grad_v.at[turn, side],
            r.out_sem.at[19 + turn],
            r.g_sem.at[turn],
            tensor=partner,
        )

    def misfit_start(turn):
        r.m_send[turn] = r.part[turn, given].astype(bf16)
        misfit_copy(turn).start()

    def double_start(turn, stage):
        if stage == 0:
            misfit_copy(turn).wait_recv()
            total = r.part[turn, kept] + r.m_land[turn].astype(f32)
            values = [total[:, :half_cols], total[:, half_cols:]]
        else:
            values = doubled(turn, stage - 1)
        for half in range(2):
            r.v_share[turn, stage, half] = values[half].astype(bf16)
            double_copy(turn, stage, half).start()

    def doubled(turn, stage):
        values = []
        for half in range(2):
            double_copy(turn, stage, half).wait_recv()
            values.append(
                r.v_share[turn, stage, half].astype(f32)
                + r.v_land[turn, stage, half].astype(f32)
            )
        return values

    def grad_start(turn):
        values = doubled(turn, bits - 1)
        for half in range(2):
            span = slice(half * half_cols, (half + 1) * half_cols)
            r.grad_v[turn, core, :, span] = (values[half] * loss_scale).astype(bf16)
        grad_copy(turn, core).start()

    out_gh = r.out_sem.at[pl.ds(12, 2)]
    grad_hidden = Chain(r.gh, r.gh_land, r.gh_share, out_gh, r.gh_sem, b, groups)

    def back(turn):
        grad_copy(turn, 1 - core).wait_recv()
        for side in range(2):
            first = turn * tall + side * short
            r.o_grad[first : first + short] = r.grad_v[turn, side]
        rows = slice(turn * tall, (turn + 1) * tall)
        for chunk in range(0, chunks, 2):
            span = slice(chunk * cols, (chunk + 2) * cols)
            value = jnp.dot(r.o_grad[rows], r.wd[:, span], preferred_element_type=f32)
            for side in range(2):
                item = turn * chunks + chunk + side
                r.gh[item] = value[:, side * cols : (side + 1) * cols]
        grad_hidden.origin(turn * chunks, (turn + 1) * chunks)

    def last(turn):
        rows = slice(turn * tall, (turn + 1) * tall)
        for chunk in range(chunks):
            item = turn * chunks + chunk
            grad_hidden.total(item)
            span = slice(chunk * cols, (chunk + 1) * cols)
            gate, up, grad = r.gu[item, 0], r.gu[item, 1], r.gh[item]
            sigma = jax.nn.sigmoid(gate)
            r.o_gate[rows, span] = (
                grad * up * sigma * (1.0 + gate * (1.0 - sigma))
            ).astype(bf16)
            r.o_up[rows, span] = (grad * gate * sigma).astype(bf16)

    def steps(chain, *items):
        for late, item in items:
            chain.step(item, bool(late))

    def order_of(first, final, skew):
        order = []
        for step in range(first, final + skew):
            if step < final:
                order.append((0, step))
            if step - skew >= first:
                order.append((1, step - skew))
        return order

    items = 2 * chunks
    order = order_of(0, items, min(5, chunks))
    late = [order.index((1, item)) + 1 for item in range(items)]

    target_home()
    gate_up.origin(chunks, items)
    steps(gate_up, *order[: late[0] - 1])
    target_relay()
    steps(gate_up, *order[late[0] - 1 : late[chunks - 3]])
    target_end()
    begin = min(items - 2, chunks + 1)
    steps(gate_up, *order[late[chunks - 3] : late[begin]])
    down(0)
    misfit_start(0)
    for stage in range(bits):
        end = min(items - 1, begin + 2)
        steps(gate_up, *order[late[begin] : late[end]])
        double_start(0, stage)
        begin = end
    steps(gate_up, *order[late[begin] :])
    down(1)
    misfit_start(1)
    grad_start(0)
    double_start(1, 0)
    back(0)

    order = order_of(0, chunks, chunks)
    late = [order.index((1, item)) + 1 for item in range(chunks)]
    steps(grad_hidden, *order[:2])
    for stage in range(1, bits):
        double_start(1, stage)
    steps(grad_hidden, *order[2 : late[0] - 1])
    grad_start(1)
    for stage in range(1, bits):
        full_sum.receive(stage - 1)
        full_sum.send(stage)
    steps(grad_hidden, *order[late[0] - 1 : late[3]])
    back(1)
    steps(grad_hidden, *order[late[3] :])
    last(0)
    steps(grad_hidden, *order_of(chunks, items, chunks))
    last(1)

    full_sum.receive(bits - 1)
    for half in range(2):
        span = slice(half * (tokens // 2), (half + 1) * (tokens // 2))
        value = full_sum.final(half).T + r.resid_v[:, span].astype(f32)
        r.o_teacher[:, span] = value.astype(bf16)

    some = pl.ds(1, chips - 1)
    sent = (
        (0, r.x_land.at[some]),
        (1, r.count_land.at[some]),
        (2, r.q_send),
        (3, r.t_send),
        (4, r.c_send),
        (8, r.z_send.at[some]),
        (9, r.p_send.at[some]),
        (14, r.v_share),
    )
    for out, array in sent:
        remote(array, array, r.out_sem.at[out], r.sq_sem.at[0], tensor=partner).wait_send()
    sq_copy.wait_send()
    row_copy.wait_send()
    for turn in range(2):
        misfit_copy(turn).wait_send()
        grad_copy(turn, core).wait_send()
    routed_sum.drain()
    target_sum.drain()
    full_sum.drain()
    gate_up.drain()
    grad_hidden.drain()


def grads_kernel(
    rows, gate, up, grad, hidden, teacher, o_gate, o_up, o_down, o_teacher, hold, sem, end_sem
):
    count, parts, tall, _ = hold.shape
    copies = [pltpu.make_async_copy(teacher, o_teacher, end_sem.at[0])]
    copies[0].start()
    terms = ((grad, hidden, o_down), (rows, gate, o_gate), (rows, up, o_up))
    for which, (left, right, out) in enumerate(terms):
        for part in range(parts):
            span = pl.ds(part * tall, tall)
            hold[which, part] = contract(left[:, span], right[...], 0, 0)
            copy = pltpu.make_async_copy(hold.at[which, part], out.at[span], sem.at[which, part])
            copy.start()
            copies.append(copy)
    for copy in copies:
        copy.wait()


def on_device(
    attn_values,
    out_weight,
    residual_t,
    projector,
    student_input,
    norm_gain,
    w_gate,
    w_up,
    w_down,
    route_index,
):
    groups, tensors = lax.axis_size("batch"), lax.axis_size("tensor")
    chips = tensors // 2
    bits = chips.bit_length() - 1
    if chips != groups or 1 << bits != chips:
        raise ValueError("mesh")
    mean_routed = student_input.shape[0] // 8
    routed = mean_routed * groups
    tokens, heads = attn_values.shape
    feats = out_weight.shape[1] // tensors
    model = projector.shape[1]
    width = student_input.shape[1]
    block, units = w_gate.shape
    slots = route_index.shape[1]
    cols = min(128, units)
    chunks = units // cols
    dma = pltpu.SemaphoreType.DMA
    moved = chips - 1
    scratch = [
        pltpu.VMEM((slots + tokens, heads), bf16),
        pltpu.VMEM((tensors, heads, feats), bf16),
        pltpu.VMEM(residual_t.shape, bf16),
        pltpu.VMEM((tensors, feats, width), bf16),
        pltpu.VMEM(student_input.shape, bf16),
        pltpu.VMEM(w_gate.shape, bf16),
        pltpu.VMEM(w_up.shape, bf16),
        pltpu.VMEM(w_down.shape, bf16),
        pltpu.VMEM(route_index.shape, route_index.dtype),
        pltpu.VMEM((1, model), f32),
        dma((8 + 2 * tensors,)),
        dma((21,)),
        pltpu.VMEM((chips, slots, feats), bf16),
        pltpu.VMEM((chips, slots, feats), bf16),
        dma((chips,)),
        pltpu.VMEM((chips, tokens, feats), bf16),
        pltpu.VMEM((chips, tokens, feats), bf16),
        pltpu.VMEM((chips, 2, slots // 2, feats), bf16),
        pltpu.VMEM((moved, 2, slots // 2, feats), bf16),
        pltpu.VMEM((chips, 2, tokens // 2, feats), bf16),
        pltpu.VMEM((moved, 2, tokens // 2, feats), bf16),
        dma((chips,)),
        dma((moved, 2)),
        dma((moved, 2)),
        pltpu.VMEM((chips, slots, width), bf16),
        pltpu.VMEM((chips, slots, width), bf16),
        pltpu.VMEM((chips, 2, slots // chips, model // 4), bf16),
        pltpu.VMEM((moved, 2, slots // chips, model // 4), bf16),
        pltpu.VMEM((slots, feats), bf16),
        pltpu.VMEM((groups, slots // chips, width), bf16),
        pltpu.VMEM((groups, slots // chips, width), bf16),
        dma((chips,)),
        dma((moved, 2)),
        dma((groups,)),
        pltpu.VMEM((chips, slots, width), bf16),
        pltpu.VMEM((slots, 128), f32),
        pltpu.VMEM((slots, 128), f32),
        pltpu.VMEM((groups, 8, 128), f32),
        dma((chips,)),
        dma((2,)),
        dma((groups,)),
        pltpu.VMEM((chips, slots, width), bf16),
        pltpu.VMEM((groups, slots, width), bf16),
        dma((groups,)),
        pltpu.VMEM((groups, routed, slots // chips), bf16),
        pltpu.VMEM((2, routed, width), bf16),
        dma((2,)),
        pltpu.VMEM((2 * chunks, 2, routed // 2, cols), f32),
        pltpu.VMEM((2, 2 * chunks, 2, routed // 2, cols), bf16),
        pltpu.VMEM((2, 2 * chunks, 2, routed // 2, cols), bf16),
        dma((2, 2 * chunks)),
        pltpu.VMEM((2 * chunks, routed // 2, cols), f32),
        pltpu.VMEM((2, 2 * chunks, routed // 2, cols), bf16),
        pltpu.VMEM((2, 2 * chunks, routed // 2, cols), bf16),
        dma((2, 2 * chunks)),
        pltpu.VMEM((2, routed // 2, block), f32),
        pltpu.VMEM((2, routed // 4, block), bf16),
        pltpu.VMEM((2, routed // 4, block), bf16),
        pltpu.VMEM((2, bits, 2, routed // 4, block // 2), bf16),
        pltpu.VMEM((2, bits, 2, routed // 4, block // 2), bf16),
        dma((2,)),
        dma((2, bits, 2)),
        pltpu.VMEM((2, 2, routed // 4, block), bf16),
        dma((2,)),
    ]
    rows, gate, up, grad, hidden, teacher = pl.pallas_call(
        functools.partial(exchange_kernel, (groups, tensors, mean_routed)),
        name="exchange",
        out_shape=(
            jax.ShapeDtypeStruct((routed, block), bf16),
            jax.ShapeDtypeStruct((routed, units), bf16),
            jax.ShapeDtypeStruct((routed, units), bf16),
            jax.ShapeDtypeStruct((routed, block), bf16),
            jax.ShapeDtypeStruct((routed, units), bf16),
            jax.ShapeDtypeStruct(residual_t.shape, bf16),
        ),
        in_specs=[HBM] * 10,
        out_specs=[VMEM] * 6,
        scratch_shapes=scratch,
        compiler_params=pltpu.CompilerParams(
            collective_id=1, has_side_effects=True, vmem_limit_bytes=VMEM_BYTES
        ),
    )(
        attn_values,
        out_weight,
        residual_t,
        projector,
        student_input,
        norm_gain.reshape(1, -1),
        w_gate,
        w_up,
        w_down,
        route_index,
    )
    parts = block // 128
    grads = jax.ShapeDtypeStruct((block, units), f32)
    grad_gate, grad_up, grad_down, teacher_hidden = pl.pallas_call(
        grads_kernel,
        name="grads",
        out_shape=(grads, grads, grads, jax.ShapeDtypeStruct(residual_t.shape, bf16)),
        in_specs=[VMEM] * 6,
        out_specs=[HBM] * 4,
        scratch_shapes=[
            pltpu.VMEM((3, parts, block // parts, units), f32),
            dma((3, parts)),
            dma((1,)),
        ],
        compiler_params=pltpu.CompilerParams(vmem_limit_bytes=20_000_000),
    )(rows, gate, up, grad, hidden, teacher)
    return (teacher_hidden, grad_gate, grad_up, grad_down)


def solution(mesh):
    in_specs = (
        P("batch", "tensor"),
        P("tensor", None),
        P("tensor", "batch"),
        P("tensor", None),
        P("batch", "tensor"),
        P(),
        P("batch", "tensor"),
        P("batch", "tensor"),
        P("batch", "tensor"),
        P("batch", None),
    )
    out_specs = (
        P("tensor", "batch"),
        P("batch", "tensor"),
        P("batch", "tensor"),
        P("batch", "tensor"),
    )
    return jax.shard_map(
        on_device, mesh=mesh, in_specs=in_specs, out_specs=out_specs, check_vma=False
    )
```
